32 devices in a mesh: rep: 1 (over z), dp: 32 (over x, y, core).
Axes of the slice: x: 4, y: 4, z: 1, core: 2. Of those that a mesh axis runs over, the one named last changes fastest.
The devices are a block of a 4x4x8 slice.
Arguments:
- x: bfloat16 [32, 2048, 640], P(('rep', 'dp'))
- dy: bfloat16 [32, 2048, 640], P(('rep', 'dp'))
- wq: bfloat16 [2, 640, 640], replicated
- wk: bfloat16 [2, 640, 128], replicated
- wv: bfloat16 [2, 640, 128], replicated
- wo: bfloat16 [2, 640, 640], replicated
- w_gate: bfloat16 [2, 640, 2048], replicated
- w_up: bfloat16 [2, 640, 2048], replicated
- w_down: bfloat16 [2, 2048, 640], replicated
- m_wq: float32 [2, 640, 640], replicated
- m_wk: float32 [2, 640, 128], replicated
- m_wv: float32 [2, 640, 128], replicated
- m_wo: float32 [2, 640, 640], replicated
- m_w_gate: float32 [2, 640, 2048], replicated
- m_w_up: float32 [2, 640, 2048], replicated
- m_w_down: float32 [2, 2048, 640], replicated
- v_wq: float32 [2, 640, 640], replicated
- v_wk: float32 [2, 640, 128], replicated
- v_wv: float32 [2, 640, 128], replicated
- v_wo: float32 [2, 640, 640], replicated
- v_w_gate: float32 [2, 640, 2048], replicated
- v_w_up: float32 [2, 640, 2048], replicated
- v_w_down: float32 [2, 2048, 640], replicated
Outputs:
- output 1: bfloat16 [2, 640, 640], P('rep')
- output 2: bfloat16 [2, 640, 128], P('rep')
- output 3: bfloat16 [2, 640, 128], P('rep')
- output 4: bfloat16 [2, 640, 640], P('rep')
- output 5: bfloat16 [2, 640, 2048], P('rep')
- output 6: bfloat16 [2, 640, 2048], P('rep')
- output 7: bfloat16 [2, 2048, 640], P('rep')
- output 8: float32 [2, 640, 640], P('rep')
- output 9: float32 [2, 640, 128], P('rep')
- output 10: float32 [2, 640, 128], P('rep')
- output 11: float32 [2, 640, 640], P('rep')
- output 12: float32 [2, 640, 2048], P('rep')
- output 13: float32 [2, 640, 2048], P('rep')
- output 14: float32 [2, 2048, 640], P('rep')
- output 15: float32 [2, 640, 640], P('rep')
- output 16: float32 [2, 640, 128], P('rep')
- output 17: float32 [2, 640, 128], P('rep')
- output 18: float32 [2, 640, 640], P('rep')
- output 19: float32 [2, 640, 2048], P('rep')
- output 20: float32 [2, 640, 2048], P('rep')
- output 21: float32 [2, 2048, 640], P('rep')
All inputs are finite; a program needn't handle non-finite values.
Results may differ from the reference program's by a relative error of at most 0.0242.
Values are sent between devices in bfloat16 or wider.
A program may use at most 768 MiB of HBM per device.

```python
import jax
import jax.numpy as jnp
from jax import lax

SEQUENCES = 32
TOKENS = 2048
D = 640
HEADS = 5
KV_HEADS = 1
HEAD = 128
FF = 2048
LAYERS = 2
THETA = 10000
NAMES = ("wq", "wk", "wv", "wo", "w_gate", "w_up", "w_down")
SHAPES = {
    "wq": (LAYERS, D, HEADS * HEAD),
    "wk": (LAYERS, D, KV_HEADS * HEAD),
    "wv": (LAYERS, D, KV_HEADS * HEAD),
    "wo": (LAYERS, HEADS * HEAD, D),
    "w_gate": (LAYERS, D, FF),
    "w_up": (LAYERS, D, FF),
    "w_down": (LAYERS, FF, D),
}


def bump(key, n, height):
    away = (jnp.arange(n, dtype=jnp.int32) - jax.random.randint(key, (), 0, n, jnp.int32)) % n
    return jnp.where(away < n // 8, height, 1.0)


def together(key, own, strength):
    shared = jax.random.normal(key, own.shape[1:], jnp.float32)
    return (own + strength * shared) * lax.rsqrt(1 + strength * strength)


def setup_inputs(seed: int = 0, part: int = 0) -> dict:
    kx, kdy, ka, kb, kz, kf, kh, kl, *keys = jax.random.split(jax.random.key(seed), 8 + 3 * len(NAMES))
    kx, kdy, ka, kb = (jax.random.fold_in(k, part) for k in (kx, kdy, ka, kb))
    kw, km, kv = (keys[i::3] for i in range(3))
    shape = (SEQUENCES, TOKENS, D)
    much_x, much_dy = jax.random.uniform(kz, (2,), jnp.float32, 0.0, 1.0)
    loud = 2.0 ** jax.random.uniform(jax.random.fold_in(kz, 1), (), jnp.float32, -1.0, 2.0)
    layers = 2.0 ** jax.random.uniform(kl, (LAYERS, 1, 1), jnp.float32, -1.0, 1.0)
    times = {"wq": 1.0, "wk": 1.0, "wv": 2.0, "wo": layers, "w_gate": 1.0, "w_up": bump(kh, FF, 4.0), "w_down": layers}
    x = together(ka, jax.random.normal(kx, shape, jnp.float32), much_x) * bump(kf, D, 4.0)
    dy = together(kb, jax.random.normal(kdy, shape, jnp.float32), much_dy)
    drawn = {"x": x.astype(jnp.bfloat16), "dy": (loud * dy * (SEQUENCES * TOKENS) ** -0.5).astype(jnp.bfloat16)}
    for key, name in zip(kw, NAMES, strict=True):
        drawn[name] = (jax.random.normal(key, SHAPES[name], jnp.float32) * SHAPES[name][1] ** -0.5 * times[name]).astype(jnp.bfloat16)
    for key, name in zip(km, NAMES, strict=True):
        drawn[f"m_{name}"] = 0.1 * jax.random.normal(key, SHAPES[name], jnp.float32)
    for key, name in zip(kv, NAMES, strict=True):
        drawn[f"v_{name}"] = jax.random.uniform(key, SHAPES[name], jnp.float32, 0.02, 0.06)
    return drawn


def matmul(a, w):
    return jnp.dot(a, w, preferred_element_type=jnp.float32).astype(jnp.bfloat16)


def normed(h):
    wide = h.astype(jnp.float32)
    scale = lax.rsqrt(jnp.mean(wide**2, -1, keepdims=True) + 1e-6)
    return (wide * scale).astype(jnp.bfloat16)


def turned(t, theta):
    half = t.shape[-1] // 2
    angle = jnp.arange(t.shape[0], dtype=jnp.float32)[:, None] * theta ** (-jnp.arange(half, dtype=jnp.float32) / half)
    cos, sin = jnp.cos(angle)[:, None], jnp.sin(angle)[:, None]
    a, b = t[..., :half].astype(jnp.float32), t[..., half:].astype(jnp.float32)
    return jnp.concatenate([a * cos - b * sin, b * cos + a * sin], -1).astype(jnp.bfloat16)


def seen_by(q, k, v):
    tokens, kv = q.shape[0], k.shape[1]
    q = q.reshape(tokens, kv, -1, q.shape[-1])
    scores = jnp.einsum("tgsd,ugd->gstu", q.astype(jnp.float32), k.astype(jnp.float32)) * q.shape[-1] ** -0.5
    place = jnp.arange(tokens)
    weights = jax.nn.softmax(jnp.where(place[:, None] >= place, scores, -jnp.inf), -1).astype(jnp.bfloat16)
    return jnp.einsum("gstu,ugd->tgsd", weights.astype(jnp.float32), v.astype(jnp.float32)).astype(jnp.bfloat16).reshape(tokens, -1)


def layer(h, w):
    a = normed(h)
    q, k = (turned(matmul(a, w[name]).reshape(h.shape[0], -1, HEAD), THETA) for name in ("wq", "wk"))
    h = h + matmul(seen_by(q, k, matmul(a, w["wv"]).reshape(h.shape[0], -1, HEAD)), w["wo"])
    b = normed(h)
    gate = jnp.dot(b, w["w_gate"], preferred_element_type=jnp.float32)
    up = jnp.dot(b, w["w_up"], preferred_element_type=jnp.float32)
    return h + matmul((jax.nn.silu(gate) * up).astype(jnp.bfloat16), w["w_down"])


def adamw(w, m, v, g):
    m = 0.9 * m + 0.1 * g
    v = 0.95 * v + 0.05 * g * g
    step = m * lax.rsqrt(v + 1e-8) + 0.1 * w
    return (w - 0.02 * step).astype(jnp.bfloat16), m, v


def clipped(gradients, sum_of_squares, count):
    factor = jnp.minimum(1.0, 0.5 * lax.rsqrt(sum_of_squares / count + 1e-30))
    return [g * factor for g in gradients]


def stack(weights, h):
    return lax.scan(lambda h, w: (layer(h, w), None), h, weights)[0]


def reference(x, dy, wq, wk, wv, wo, w_gate, w_up, w_down, m_wq, m_wk, m_wv, m_wo, m_w_gate, m_w_up, m_w_down, v_wq, v_wk, v_wv, v_wo, v_w_gate, v_w_up, v_w_down):
    weights = dict(zip(NAMES, (wq, wk, wv, wo, w_gate, w_up, w_down), strict=True))

    def take(so_far, sequence):
        h, by_y = sequence
        _, back = jax.vjp(stack, weights, h)
        by_weights, by_h = back(by_y)
        return jax.tree.map(lambda total, term: total + term.astype(jnp.float32), so_far, by_weights), by_h

    none_yet = {name: jnp.zeros(w.shape, jnp.float32) for name, w in weights.items()}
    by_weights, by_x = lax.scan(take, none_yet, (x, dy))
    gradients = [by_weights[name].astype(jnp.bfloat16).astype(jnp.float32) for name in NAMES]
    gradients = clipped(gradients, sum(jnp.sum(g * g) for g in gradients), sum(g.size for g in gradients))
    first = (m_wq, m_wk, m_wv, m_wo, m_w_gate, m_w_up, m_w_down)
    second = (v_wq, v_wk, v_wv, v_wo, v_w_gate, v_w_up, v_w_down)
    new = [adamw(weights[name].astype(jnp.float32), m, v, g) for name, m, v, g in zip(NAMES, first, second, gradients, strict=True)]
    return tuple(one[which] for which in range(3) for one in new)
```

```python
import functools

import jax
import jax.numpy as jnp
import numpy as np
from jax import lax
from jax.experimental import pallas as pl
from jax.experimental.pallas import tpu as pltpu
from jax.sharding import PartitionSpec as P

BF, F32 = jnp.bfloat16, jnp.float32
MESH = pl.DeviceIdType.MESH
HEAD = LANES = 128
HALF = HEAD // 2
THETA = 10000
SIDE = 4
CORES = COLOURS = 2
PIECES = CORES * COLOURS * SIDE * SIDE
WAYS = CORES * COLOURS
TILE = 16
LOG2E = 1.4426950408889634
NEG = -1e30
HIDDEN = NEG + NEG
BLOCK = 512
FINE = 256
AHEAD = 2
PARTS = 2
READY = 6
MEMORY = 63 * 2**20
ONE = 1.0
ANY = pl.BlockSpec(memory_space=pl.ANY)
HERE = pl.BlockSpec(memory_space=pltpu.VMEM)
HBM = pl.BlockSpec(memory_space=pltpu.HBM)


def dot(a, b, ca=1, cb=0):
    return lax.dot_general(a, b, (((ca,), (cb,)), ((), ())), preferred_element_type=F32)


dot_first = functools.partial(dot, ca=0, cb=0)
dot_last = functools.partial(dot, ca=1, cb=1)


def bf(t):
    return t.astype(BF)


def wide(t):
    return t.astype(F32)


def at(n, size):
    return pl.ds(pl.multiple_of(n * size, size), size)


def get(ref):
    return ref[...]


def vmem(*shape, dtype=BF):
    return pltpu.VMEM(shape, dtype)


def array(*shape, dtype=BF):
    return jax.ShapeDtypeStruct(shape, dtype)


def whole(*shape):
    return pl.BlockSpec(shape, lambda i: (0,) * len(shape), pipeline_mode=pl.Buffered(1))


def cols(rows, size, of):
    return pl.BlockSpec((rows, size), lambda i: (0, of(i)))


def tiles(rows, size, of):
    return pl.BlockSpec((None, None, rows, size), lambda i: (*of(i), 0))


def within(i, first, count):
    return jnp.clip(i - first, 0, count - 1)


def mean_square(w):
    return lax.rsqrt(jnp.mean(w * w, 0, keepdims=True) + 1e-6)


def normed(h):
    return bf(wide(h) * mean_square(wide(h)))


def norm_bwd(h, d, dh):
    w, d = wide(h), wide(bf(d))
    r = mean_square(w)
    return bf(wide(dh) + wide(bf(r * (d - w * (r * r * jnp.mean(d * w, 0, keepdims=True))))))


def rotary(tokens):
    angle = np.arange(tokens, dtype=np.float32) * (np.float32(THETA) ** (-np.arange(HALF, dtype=np.float32) / np.float32(HALF)))[:, None]
    return np.concatenate([np.cos(angle), np.sin(angle)]).astype(np.float32)


def turned(t, tab, back=False):
    t = wide(t)
    a, b, c, s = t[:HALF], t[HALF:], tab[:HALF], tab[HALF:]
    s = -s if back else s
    return bf(jnp.concatenate([a * c - b * s, b * c + a * s]))


def gap(ref):
    ref[...] = lax.broadcasted_iota(jnp.int32, ref.shape, 1) - lax.broadcasted_iota(jnp.int32, ref.shape, 0)


def kept_in(space, *arrays):
    return [pltpu.with_memory_space_constraint(a, space) for a in arrays]


class Loads:
    def __init__(self, pairs, sems, first):
        self.copies = [pltpu.make_async_copy(a, b, sems.at[first + n]) for n, (a, b) in enumerate(pairs)]

    def start(self):
        for copy in self.copies:
            copy.start()

    def wait(self):
        for copy in self.copies:
            copy.wait()


def params(collective=None):
    extra = {} if collective is None else dict(collective_id=collective, has_side_effects=True)
    return pltpu.CompilerParams(dimension_semantics=("arbitrary",), vmem_limit_bytes=MEMORY, **extra)


def cost(flops):
    return pl.CostEstimate(flops=flops, transcendentals=0, bytes_accessed=2**25)


def on(step, first, count):
    def run(body):
        pl.when((step >= first) & (step < first + count))(lambda: body(step - first))

    return run


def _forward(x_ref, tab_ref, *refs, layers, heads, blocks, steps):
    wq, wk, wv, wo, wg, wu, wd = refs[:7]
    h_ref, a_ref, q_ref, kv_ref, o_ref, lse_ref, h2_ref, b_ref, silu_ref, slope_ref, act_ref = refs[7:18]
    h_s, q_s, k_s, v_s, o_s, top_s, mix_s, gap_s, b_s, act_s, gate_s, up_s, down_s, wq_s, wk_s, wv_s, wo_s, wg_s, wu_s, wd_s, sems = refs[18:]
    step = pl.program_id(0)
    per = 2 * blocks + steps
    layer, s = lax.div(step, per), lax.rem(step, per)
    early = lambda n: Loads([(w.at[n], t) for w, t in ((wq, wq_s), (wk, wk_s), (wv, wv_s))], sems, 0)
    late = lambda n: Loads([(w.at[n], t) for w, t in ((wo, wo_s), (wg, wg_s), (wu, wu_s), (wd, wd_s))], sems, 3)

    @pl.when(step == 0)
    def _():
        early(layer).start()
        gap(gap_s)
        v_s[HEAD:, :] = jnp.ones_like(v_s[HEAD:, :])

    @pl.when(s == 0)
    def _():
        early(layer).wait()
        late(layer).start()

    @on(s, 0, blocks)
    def _(n):
        here = at(n, BLOCK)

        @pl.when(layer == 0)
        def _():
            h_s[:, here] = get(x_ref).T

        h_ref[...] = h_s[:, here]
        a, tab = normed(h_s[:, here]), get(tab_ref)
        a_ref[...] = a
        q = bf(dot_first(get(wq_s), a))
        for head in range(heads):
            rows = slice(head * HEAD, head * HEAD + HEAD)
            q_s[rows, here] = turned(q[rows], tab)
        q_ref[...] = q_s[:, here]
        k, v = turned(bf(dot_first(get(wk_s), a)), tab), bf(dot_first(get(wv_s), a))
        k_s[here, :] = k.T
        v_s[:HEAD, here] = v
        kv_ref[:HEAD, :], kv_ref[HEAD:, :] = k, v

    @pl.when((s == blocks) & (layer < layers - 1))
    def _():
        early(layer + 1).start()

    @on(s, blocks, blocks)
    def _(n):
        pl.when(n == 0)(late(layer).wait)
        scale = HEAD**-0.5
        e = scale * LOG2E
        top_s[...] = jnp.full(top_s.shape, NEG, F32)
        mix_s[...] = jnp.zeros(mix_s.shape, F32)

        def block(first, size, skip, masked):
            here = pl.ds(pl.multiple_of(first, size), size)
            queries = pl.ds(pl.multiple_of(n * BLOCK + skip, size), BLOCK - skip)
            keys, values = k_s[here, :], v_s[:, here]
            scores = [dot(keys, q_s[head * HEAD : head * HEAD + HEAD, queries]) for head in range(heads)]
            weights, keeps = [], []
            for head, score in enumerate(scores):
                if masked:
                    score = jnp.where(gap_s[:, : BLOCK - skip] >= 0, score, HIDDEN)
                row = slice(head, head + 1)
                old = top_s[row, skip:]
                top = jnp.maximum(old, score.max(axis=0, keepdims=True))
                top_s[row, skip:] = top
                weights.append(bf(jnp.exp2((score - top) * e)))
                keeps.append(jnp.exp2((old - top) * e))
            for head in range(heads):
                mix_s[head, :, skip:] = mix_s[head, :, skip:] * keeps[head] + dot(values, weights[head])

        lax.fori_loop(0, n, lambda j, _: block(j * BLOCK, BLOCK, 0, False), None)
        part = at(n, wg_s.shape[1] // blocks)
        gate_s[part, :], up_s[part, :], down_s[:, part] = wg_s[:, part].T, wu_s[:, part].T, wd_s[part, :].T
        for skip in range(0, BLOCK, FINE):
            block(n * BLOCK + skip, FINE, skip, True)
        for head in range(heads):
            row, rows = slice(head, head + 1), slice(head * HEAD, head * HEAD + HEAD)
            total = mix_s[head, HEAD : HEAD + 1, :]
            o_ref[rows, :] = bf(mix_s[head, :HEAD, :] * (ONE / total))
            lse_ref[row, :] = top_s[row, :] * scale + jnp.log(total)
        o_s[:, at(n, BLOCK)] = get(o_ref)

    @on(s, 2 * blocks, steps)
    def _(n):
        here, part, size = at(lax.div(n, PARTS), BLOCK), lax.rem(n, PARTS), wg_s.shape[1] // PARTS

        @pl.when(part == 0)
        def _():
            h2 = bf(wide(h_s[:, here]) + wide(bf(dot_first(get(wo_s), o_s[:, here]))))
            h_s[:, here], h2_ref[...] = h2, h2
            b = normed(h2)
            b_s[...], b_ref[...] = b, b

        for c in range(0, size, BLOCK):
            mine, all_ = slice(c, c + BLOCK), pl.ds(pl.multiple_of(part * size + c, BLOCK), BLOCK)
            gate, up = dot(gate_s[all_, :], get(b_s)), dot(up_s[all_, :], get(b_s))
            sig = 0.5 * jnp.tanh(0.5 * gate) + 0.5
            silu = gate * sig
            silu_ref[mine, :] = silu
            slope_ref[mine, :] = up * (sig + silu * (ONE - sig))
            act = bf(silu * up)
            act_s[all_, :], act_ref[mine, :] = act, act

        @pl.when((part == PARTS - 1) & (layer < layers - 1))
        def _():
            h_s[:, here] = bf(wide(h_s[:, here]) + wide(bf(dot(get(down_s), get(act_s)))))


def forward(x, tab, wq, wk, wv, wo, wg, wu, wd):
    (t, d), (layers, _, ff) = x.shape, wg.shape
    heads, blocks, steps, kv = d // HEAD, t // BLOCK, t // BLOCK * PARTS, HEAD + HEAD
    per = 2 * blocks + steps
    phase = lambda first, count: lambda i: (lax.div(i, per), within(lax.rem(i, per), first, count))
    qkv, att = phase(0, blocks), phase(blocks, blocks)

    def mlp(i, parts):
        layer, n = phase(2 * blocks, steps)(i)
        return layer, lax.div(n, PARTS), lax.rem(n, parts)

    small, big = lambda rows, of: pl.BlockSpec((None, rows, BLOCK), lambda i: (of(i)[0], 0, of(i)[1])), lambda rows, parts=1: tiles(rows // parts, BLOCK, lambda i: mlp(i, parts))
    make, make_big = lambda rows, dtype=BF: array(layers, rows, t, dtype=dtype), lambda rows, dtype=BF: array(layers, blocks, rows, BLOCK, dtype=dtype)
    return pl.pallas_call(
        functools.partial(_forward, layers=layers, heads=heads, blocks=blocks, steps=steps),
        name="forward",
        grid=(layers * per,),
        in_specs=[pl.BlockSpec((BLOCK, d), lambda i: (within(i, 0, blocks), 0)), cols(HEAD, BLOCK, lambda i: qkv(i)[1])] + [ANY] * 7,
        out_specs=[small(d, qkv), small(d, qkv), small(d, qkv), small(kv, qkv), small(d, att), small(heads, att), big(d), big(d), big(ff, PARTS), big(ff, PARTS), big(ff, PARTS)],
        out_shape=[make(d), make(d), make(d), make(kv), make(d), make(heads, F32), make_big(d), make_big(d), make_big(ff, F32), make_big(ff, F32), make_big(ff)],
        scratch_shapes=[vmem(d, t), vmem(d, t), vmem(t, HEAD), vmem(HEAD + TILE // 2, t), vmem(d, t), vmem(heads, BLOCK, dtype=F32),
                        vmem(heads, HEAD + TILE // 2, BLOCK, dtype=F32), vmem(FINE, BLOCK, dtype=jnp.int32), vmem(d, BLOCK), vmem(ff, BLOCK), vmem(ff, d), vmem(ff, d), vmem(d, ff)]
        + [vmem(*w.shape[1:]) for w in (wq, wk, wv, wo, wg, wu, wd)] + [pltpu.SemaphoreType.DMA((7,))],
        compiler_params=params(),
        cost_estimate=cost(2 * layers * t * d * (d + d + kv + t + 3 * ff)),
    )(x, tab, wq, wk, wv, wo, wg, wu, wd)


FAR = (2, 1, 3)
NEAR = (1, 3)


def halves(up, first):
    return slice(2, SIDE) if up == first else slice(0, 2)


class Place:
    def __init__(self):
        me = lax.axis_index("dp")
        self.core = lax.rem(me, CORES)
        self.places = lax.div(me, SIDE * CORES), lax.rem(lax.div(me, CORES), SIDE)

    def device(self, places, core):
        return {"dp": (places[0] * SIDE + places[1]) * CORES + core}

    def partner(self):
        return self.device(self.places, 1 - self.core)

    def along(self, axis, far):
        return self.device([lax.rem(p + far, SIDE) if n == axis else p for n, p in enumerate(self.places)], self.core)

    def greet(self):
        barrier = pltpu.get_barrier_semaphore()
        peers = [self.partner()] + [self.along(axis, far) for axis in range(COLOURS) for far in FAR]
        for peer in peers:
            pl.semaphore_signal(barrier, inc=1, device_id=peer, device_id_type=MESH)
        pl.semaphore_wait(barrier, len(peers))


def send(src, dst, sems, index, to):
    return pltpu.make_async_remote_copy(src_ref=src, dst_ref=dst, send_sem=sems.at[(0, *index)], recv_sem=sems.at[(1, *index)], device_id=to, device_id_type=MESH)


def add(dst, parts):
    rows = dst.shape[0]
    size = max(n for n in range(TILE, min(FINE, rows) + 1, TILE) if rows % n == 0)

    def body(n, _):
        here = at(n, size)
        dst[here, :] = bf(sum(wide(p[here, :]) for p in parts[1:]) + wide(parts[0][here, :]))
        return _

    lax.fori_loop(0, rows // size, body, 0)


def semaphores(*shape):
    return pltpu.SemaphoreType.DMA(shape)


class Reduce:
    @staticmethod
    def scratch(rows):
        half = vmem(COLOURS, SIDE, SIDE, rows, LANES)
        return [half, half, vmem(COLOURS, SIDE, SIDE, rows, LANES), vmem(COLOURS, SIDE, rows, LANES), semaphores(COLOURS, SIDE),
                semaphores(2, COLOURS, SIDE), semaphores(2, COLOURS, SIDE, 2), semaphores(2, COLOURS, SIDE)]

    def __init__(self, place, pieces, shard, scratch):
        self.place, self.pieces, self.shard = place, pieces, shard
        self.own, self.other, self.one, self.two, self.s_own, self.s_core, self.s_one, self.s_two = scratch
        self.order = [[(far, lax.rem(p + far, SIDE)) for far in (*FAR, 0)] for p in place.places]

    def cores(self, colour, far, n):
        core = self.place.core
        return (send(self.pieces.at[1 - core, colour, n], self.other.at[colour, n], self.s_core, (colour, far), self.place.partner()),
                pltpu.make_async_copy(self.pieces.at[core, colour, n], self.own.at[colour, n], self.s_own.at[colour, far]))

    def near(self, colour, far, first):
        half = halves(far == 1, first)
        n = lax.rem(self.place.places[colour] + far, SIDE)
        return send(self.own.at[colour, n, half], self.one.at[colour, far, half], self.s_one, (colour, far, int(first)), self.place.along(colour, far))

    def across(self, colour, far):
        half = halves(far == 1, False)
        n = lax.rem(self.place.places[colour] + 2, SIDE)
        return send(self.own.at[colour, n, half], self.one.at[colour, 2, half], self.s_one, (colour, 2, int(far == 1)), self.place.along(colour, far))

    def seconds(self, colour, far, n):
        return send(self.own.at[colour, self.place.places[colour], n], self.two.at[colour, far], self.s_two, (colour, far), self.place.along(1 - colour, far))

    def chunks(self, axis_of):
        return [(colour, *self.order[axis_of(colour)][n]) for n in range(SIDE) for colour in range(COLOURS)]

    def start(self):
        for chunk in self.chunks(lambda colour: colour):
            for copy in self.cores(*chunk):
                copy.start()

    def first(self):
        for colour, far, n in self.chunks(lambda colour: colour):
            for copy in self.cores(colour, far, n):
                copy.wait()
            for m in range(SIDE):
                add(self.own.at[colour, n, m], [self.own.at[colour, n, m], self.other.at[colour, n, m]])
            for neighbour in NEAR:
                if far == 2:
                    self.across(colour, neighbour).start()
                if far == neighbour:
                    self.near(colour, far, True).start()

    def relay(self):
        for colour in range(COLOURS):
            for far in NEAR:
                self.across(colour, far).wait()
                n = lax.rem(self.place.places[colour] + far, SIDE)
                for m in range(SIDE)[halves(far == 1, False)]:
                    add(self.own.at[colour, n, m], [self.own.at[colour, n, m], self.one.at[colour, 2, m]])
                self.near(colour, far, False).start()

    def second(self):
        for colour in range(COLOURS):
            for far in NEAR:
                for first in (True, False):
                    self.near(colour, far, first).wait()
        for colour, far, n in self.chunks(lambda colour: 1 - colour):
            mine = self.own.at[colour, self.place.places[colour], n]
            add(mine, [mine] + [self.one.at[colour, f, n] for f in NEAR])
            if far:
                self.seconds(colour, far, n).start()

    def third(self):
        for colour, far, n in self.chunks(lambda colour: 1 - colour):
            if far:
                self.seconds(colour, far, n).wait()
        for colour in range(COLOURS):
            mine = self.own.at[colour, self.place.places[colour], self.place.places[1 - colour]]
            add(self.shard.at[colour], [mine] + [self.two.at[colour, f] for f in FAR])

    def stages(self):
        return [self.start, self.first, self.relay, self.second, self.third]


class Gather:
    @staticmethod
    def scratch(rows):
        return [semaphores(COLOURS), semaphores(2, COLOURS, SIDE), semaphores(2, COLOURS, SIDE, 2), semaphores(2, COLOURS, SIDE)]

    def __init__(self, place, shard, pieces, scratch):
        self.place, self.shard, self.pieces = place, shard, pieces
        self.s_own, self.s_two, self.s_one, self.s_core = scratch

    def place_of(self, colour):
        places = self.place.places
        return self.pieces.at[self.place.core, colour, places[colour], places[1 - colour]]

    def owns(self, colour):
        return pltpu.make_async_copy(self.shard.at[colour], self.place_of(colour), self.s_own.at[colour])

    def seconds(self, colour, far):
        return send(self.shard.at[colour], self.place_of(colour), self.s_two, (colour, far), self.place.along(1 - colour, far))

    def behind(self, colour, far):
        return lax.rem(self.place.places[colour] + SIDE - far, SIDE)

    def near(self, colour, far):
        here = self.pieces.at[self.place.core, colour, self.place.places[colour]]
        return send(here, here, self.s_one, (colour, far, 0), self.place.along(colour, far))

    def across(self, colour, far):
        here = self.pieces.at[self.place.core, colour, self.behind(colour, far), halves(far == 1, True)]
        return send(here, here, self.s_one, (colour, far, 1), self.place.along(colour, far))

    def cores(self, colour, far):
        here = self.pieces.at[self.place.core, colour, self.behind(colour, far)]
        return send(here, here, self.s_core, (colour, far), self.place.partner())

    def start(self):
        for colour in range(COLOURS):
            for far in FAR:
                self.seconds(colour, far).start()
            self.owns(colour).start()

    def first(self):
        for colour in range(COLOURS):
            self.owns(colour).wait()
            for far in FAR:
                self.seconds(colour, far).wait()
            for far in NEAR:
                self.near(colour, far).start()
            self.cores(colour, 0).start()

    def relay(self):
        for colour in range(COLOURS):
            for far in NEAR:
                self.near(colour, far).wait()
                self.across(colour, far).start()
                self.cores(colour, far).start()

    def second(self):
        for colour in range(COLOURS):
            for far in NEAR:
                self.across(colour, far).wait()
            self.cores(colour, 2).start()

    def finish(self):
        for far in (0, *FAR):
            for colour in range(COLOURS):
                self.cores(colour, far).wait()

    def stages(self):
        return [self.start, self.first, self.relay, self.second, self.finish]


class Comm:
    def __init__(self, pieces, points):
        self.pieces, self.points = pieces, points

    def outs(self):
        rows = self.pieces.shape[-2]
        shard = (COLOURS, rows, LANES)
        return ([pl.BlockSpec(shard, lambda i: (0,) * len(shard)), ANY], [array(*shard), array(*self.pieces.shape)], Reduce.scratch(rows) + Gather.scratch(rows))

    def plan(self, pieces, shard, back, *scratch):
        place, n = Place(), len(Reduce.scratch(TILE))
        stages = Reduce(place, pieces, shard, scratch[:n]).stages() + Gather(place, shard, back, scratch[n:]).stages()
        return [(0, place.greet), *zip(self.points, stages, strict=True)]

    def host(self, kernel, opening, n_in, n_out):
        specs, _, scratch = self.outs()

        def body(*refs):
            refs, step = list(refs), pl.program_id(0)
            take = lambda n: [refs.pop(0) for _ in range(n)]
            ins, (pieces,), outs, (shard, back) = take(n_in), take(1), take(n_out), take(len(specs))
            own, found = take(len(refs) - len(scratch)), self.plan(pieces, shard, back, *refs[-len(scratch) :])

            def run(end):
                for point in sorted({p for p, _ in found}):
                    if (point < 0) == end:
                        @pl.when(step == abs(point) - end)
                        def _():
                            for p, stage in found:
                                if p == point:
                                    stage()

            if opening:
                pl.when(step == 0)(lambda: opening(*ins, *outs, *own))
            run(False)
            kernel(*ins, *outs, *own)
            run(True)

        return body


def call(kernel, comm, cid, *, name, grid, in_specs, out_specs, out_shape, scratch_shapes, args, flops, opening=None):
    if comm is not None:
        specs, shapes, scratch = comm.outs()
        kernel = comm.host(kernel, opening, len(in_specs), len(out_specs))
        in_specs, out_specs, out_shape = in_specs + [ANY], out_specs + specs, out_shape + shapes
        scratch_shapes, args = scratch_shapes + scratch, (*args, comm.pieces)
    return pl.pallas_call(kernel, name=name, grid=grid, in_specs=in_specs, out_specs=out_specs, out_shape=out_shape, scratch_shapes=scratch_shapes,
                          compiler_params=params(None if comm is None else cid), cost_estimate=cost(flops))(*args)


def squares(shard):
    def body(n, total):
        here = at(n, TILE)
        return total + sum(wide(shard[colour, here, :]) * wide(shard[colour, here, :]) for colour in range(COLOURS))

    return lax.fori_loop(0, shard.shape[1] // TILE, body, jnp.zeros((TILE, LANES), F32))


def _gradients(dy_ref, silu_ref, slope_ref, b_ref, act_ref, wd_ref, dg_ref, du_ref, grad_ref, gate_s, up_s, down_s, dy_s, *, flip, steps):
    step = pl.program_id(0)

    @on(step, 0, steps)
    def _(n):
        part, size = lax.rem(n, PARTS), silu_ref.shape[0]

        @pl.when(part == 0)
        def _():
            dy_s[...] = get(dy_ref).T if flip else get(dy_ref)

        def work(first):
            for c in range(0, size, BLOCK):
                mine, all_ = slice(c, c + BLOCK), pl.ds(pl.multiple_of(part * size + c, BLOCK), BLOCK)
                d = wide(bf(dot(wd_ref[all_, :], get(dy_s))))
                dg_ref[mine, :], du_ref[mine, :] = bf(d * slope_ref[mine, :]), bf(d * silu_ref[mine, :])
                for total, a, other in ((gate_s, b_ref, dg_ref), (up_s, b_ref, du_ref), (down_s, dy_s, act_ref)):
                    got = dot_last(get(a), other[mine, :])
                    total[:, all_] = got if first else total[:, all_] + got

        pl.when(n < PARTS)(lambda: work(True))
        pl.when(n >= PARTS)(lambda: work(False))

    @pl.when(step == steps)
    def _():
        d, q, few = down_s.shape[0], down_s.shape[0] // WAYS, LANES // WAYS

        def body(c, _):
            columns = at(c, LANES)
            to = grad_ref.at[:, :, lax.div(c, SIDE), lax.rem(c, SIDE)]
            got = down_s[:, columns].T
            for way in range(WAYS):
                piece = to.at[way // COLOURS, way % COLOURS]
                for z, total in enumerate((gate_s, up_s)):
                    piece[z * q : z * q + q, :] = bf(total[way * q : way * q + q, columns])
                for l in range(d // LANES):
                    piece[2 * q + l * few : 2 * q + l * few + few, :] = bf(got[way * few : way * few + few, l * LANES : l * LANES + LANES])
            return _

        lax.fori_loop(0, down_s.shape[1] // LANES, body, 0)


def gradients(dy, silu, slope, b, act, wd, layer, flip, comm, cid):
    _, blocks, ff, _ = silu.shape
    d, steps = wd.shape[2], blocks * PARTS
    now, half = lambda i: lax.div(within(i, 0, steps), PARTS), lambda i: lax.rem(within(i, 0, steps), PARTS)
    once = tiles(ff // PARTS, BLOCK, lambda i: (layer, now(i), half(i)))
    mine = pl.BlockSpec((None, ff // PARTS, BLOCK), lambda i: (now(i), half(i), 0))
    grad = (CORES, COLOURS, SIDE, SIDE, 3 * d // WAYS, LANES)
    return call(
        functools.partial(_gradients, flip=flip, steps=steps), comm, cid, name="gradients", grid=(steps + 1,),
        in_specs=[pl.BlockSpec((BLOCK, d), lambda i: (now(i), 0)) if flip else cols(d, BLOCK, now), once, once, tiles(d, BLOCK, lambda i: (layer, now(i), 0)),
                  once, pl.BlockSpec((None, ff, d), lambda i: (layer, 0, 0), pipeline_mode=pl.Buffered(1))],
        out_specs=[mine, mine, pl.BlockSpec(grad, lambda i: (0,) * len(grad), pipeline_mode=pl.Buffered(1))],
        out_shape=[array(blocks, ff, BLOCK), array(blocks, ff, BLOCK), array(*grad)],
        scratch_shapes=[vmem(d, ff, dtype=F32)] * 3 + [vmem(d, BLOCK)],
        args=(dy, silu, slope, b, act, wd), flops=8 * blocks * BLOCK * d * ff,
    )


def _loads(refs, layer):
    a, o, _, wo, wg, wu, wq, wk, wv = refs[10:19]
    *_, a_s, o_s, wo_s, wg_s, wu_s, wq_s, wk_s, wv_s, sems = refs
    pairs = [(r.at[layer], s) for r, s in ((wg, wg_s), (wu, wu_s), (wo, wo_s), (wq, wq_s), (wk, wk_s), (wv, wv_s), (a, a_s), (o, o_s))]
    return Loads(pairs[:3], sems, 0), Loads(pairs[3:], sems, 3)


def _open(*refs, layer):
    for loads in _loads(refs, layer):
        loads.start()


def _backward(*refs, flip, last, heads, steps, blocks, layer):
    first, rest = _loads(refs, layer)
    dg_ref, du_ref, h2_ref, dy_ref, q_ref, kv_ref, o_ref, lse_ref, tab_ref, tabs_ref, _, _, h = refs[:13]
    outs, refs = (refs[19:20], refs[20:]) if last else (refs[19:21], refs[21:])
    dh2_s, do_s, dq_s, dkv_s, k_s, v_s, acc_s, delta_s, dk_s, dv_s, gap_s, db_s, a_s, o_s, wo_s, wg_s, wu_s, wq_s, wk_s, wv_s, _ = refs
    step = pl.program_id(0)
    pairs = blocks * (blocks + 1) // 2
    @pl.when(step == 0)
    def _():
        gap(gap_s)
        k_s[...], v_s[...] = kv_ref[:HEAD, :].T, kv_ref[HEAD:, :].T
        dk_s[...], dv_s[...] = jnp.zeros_like(dk_s), jnp.zeros_like(dv_s)
        first.wait()

    @on(step, 0, steps)
    def _(n):
        here, part = at(lax.div(n, PARTS), BLOCK), at(lax.rem(n, PARTS), dg_ref.shape[0])
        db = dot(wg_s[:, part], get(dg_ref)) + dot(wu_s[:, part], get(du_ref))

        @pl.when(lax.rem(n, PARTS) == 0)
        def _():
            db_s[...] = db

        @pl.when(lax.rem(n, PARTS) > 0)
        def _():
            dh2 = norm_bwd(get(h2_ref), db + get(db_s), get(dy_ref).T if flip else get(dy_ref))
            dh2_s[:, here] = dh2
            do_s[:, here] = bf(dot(get(wo_s), dh2))

    @on(step, steps, pairs)
    def _(n):
        iq = query_block(n, blocks)
        j = n - lax.div(iq * (iq + 1), 2)
        scale = HEAD**-0.5
        e = scale * LOG2E
        mine = at(iq, BLOCK)
        rows = [slice(head * HEAD, head * HEAD + HEAD) for head in range(heads)]

        @pl.when(j == 0)
        def _():
            acc_s[...] = jnp.zeros_like(acc_s)
            for head, r in enumerate(rows):
                delta_s[head : head + 1, :] = (wide(do_s[r, mine]) * wide(o_ref[r, :])).sum(axis=0, keepdims=True)

        def block(start, size, skip, masked):
            here = pl.ds(pl.multiple_of(start, size), size)
            queries = pl.ds(pl.multiple_of(iq * BLOCK + skip, size), BLOCK - skip)
            keys, values, turned_keys = k_s[here, :], v_s[here, :], kv_ref[:HEAD, here]
            qs, dos, pairs_ = [q_ref[r, skip:] for r in rows], [do_s[r, queries] for r in rows], []
            for head in range(heads):
                for n in range(len(pairs_), min(head + AHEAD, heads)):
                    pairs_.append((dot(keys, qs[n]), dot(values, dos[n])))
                score, dp = pairs_[head]
                p = jnp.exp2(score * e - lse_ref[head : head + 1, skip:] * LOG2E)
                if masked:
                    p = jnp.where(gap_s[:, : BLOCK - skip] >= 0, p, 0.0)
                ds = bf(p * (dp - delta_s[head : head + 1, skip:]))
                dv_s[here, :] += dot_last(bf(p), dos[head])
                dk_s[here, :] += dot_last(ds, qs[head])
                acc_s[head, :, skip:] += dot(turned_keys, ds)

        pl.when(j < iq)(lambda: block(j * BLOCK, BLOCK, 0, False))

        @pl.when(j == iq)
        def _():
            for skip in range(0, BLOCK, FINE):
                block(iq * BLOCK + skip, FINE, skip, True)
            for head, r in enumerate(rows):
                dq_s[r, mine] = turned(bf(acc_s[head] * scale), get(tab_ref), True)

        @pl.when(n == pairs - 1)
        def _():
            dkv_s[:HEAD, :] = turned(bf((get(dk_s) * scale).T), get(tabs_ref), True)
            dkv_s[HEAD:, :] = bf(get(dv_s).T)
            rest.wait()

    if not last:
        @on(step, steps + pairs, blocks)
        def _(n):
            here = at(n, BLOCK)
            da = dot(get(wq_s), dq_s[:, here]) + dot(get(wk_s), dkv_s[:HEAD, here]) + dot(get(wv_s), dkv_s[HEAD:, here])
            outs[0][...] = norm_bwd(get(h), da, dh2_s[:, here])

    @pl.when(step == pl.num_programs(0) - 1)
    def _():
        grad_ref, n = outs[-1], 0
        for got in (dot_last(get(o_s), get(dh2_s)), dot_last(get(a_s), get(dq_s)), dot_last(get(a_s), get(dkv_s))):
            for c in range(0, got.shape[1], LANES):
                for r in range(0, got.shape[0], LANES):
                    grad_ref[n] = bf(got[r : r + LANES, c : c + LANES])
                    n += 1
        for n in range(n, PIECES):
            grad_ref[n] = jnp.zeros_like(grad_ref[n])


def query_block(n, blocks):
    return sum(jnp.where(n >= b * (b + 1) // 2, 1, 0) for b in range(1, blocks))


def backward(dg, du, dy, tab, kept, weights, layer, flip, last, comm, cid):
    a, q, kv, o, lse, h2, h = kept
    wq, wk, wv, wo, wg, wu = weights
    (_, d, t), ff = q.shape, dg.shape[1]
    heads, steps, blocks = d // HEAD, t // BLOCK * PARTS, t // BLOCK
    pairs = blocks * (blocks + 1) // 2
    more = 0 if last else blocks
    now, half = lambda i: lax.div(within(i, 0, steps), PARTS), lambda i: lax.rem(within(i, 0, steps), PARTS)
    block = lambda i: query_block(within(i, steps, pairs), blocks)
    then = lambda i: within(i, steps + pairs, blocks)
    hidden = pl.BlockSpec((None, ff // PARTS, BLOCK), lambda i: (now(i), half(i), 0))
    part = lambda rows, of: pl.BlockSpec((None, rows, BLOCK), lambda i: (layer, 0, of(i)))
    out_specs, out_shape = [pl.BlockSpec((PIECES, LANES, LANES), lambda i: (0, 0, 0))], [array(PIECES, LANES, LANES)]
    if not last:
        out_specs, out_shape = [cols(d, BLOCK, then)] + out_specs, [array(d, t)] + out_shape
    got = call(
        functools.partial(_backward, flip=flip, last=last, heads=heads, steps=steps, blocks=blocks, layer=layer), comm, cid, name="backward", opening=functools.partial(_open, layer=layer),
        grid=(steps + pairs + more + 1,),
        in_specs=[hidden, hidden, tiles(d, BLOCK, lambda i: (layer, now(i), 0)), pl.BlockSpec((BLOCK, d), lambda i: (now(i), 0)) if flip else cols(d, BLOCK, now),
                  part(d, block), pl.BlockSpec((None, *kv.shape[1:]), lambda i: (layer, 0, 0), pipeline_mode=pl.Buffered(1)), part(d, block), part(heads, block),
                  cols(HEAD, BLOCK, block), whole(HEAD, t), ANY, ANY, part(d, then)] + [ANY] * 6,
        out_specs=out_specs, out_shape=out_shape,
        scratch_shapes=[vmem(d, t), vmem(d, t), vmem(d, t), vmem(HEAD + HEAD, t), vmem(t, HEAD), vmem(t, HEAD), vmem(heads, HEAD, BLOCK, dtype=F32), vmem(heads, BLOCK, dtype=F32),
                        vmem(t, HEAD, dtype=F32), vmem(t, HEAD, dtype=F32), vmem(FINE, BLOCK, dtype=jnp.int32), vmem(d, BLOCK, dtype=F32), vmem(d, t), vmem(d, t)]
        + [vmem(*w.shape[1:]) for w in (wo, wg, wu, wq, wk, wv)] + [pltpu.SemaphoreType.DMA((8,))],
        args=(dg, du, h2, dy, q, kv, o, lse, tab, tab, a, o, h, wo, wg, wu, wq, wk, wv), flops=4 * t * d * (ff + t + d),
    )
    return (None if last else got[0]), got[0 if last else 1], got[1 if last else 2 :]


def stepped(w, m, v, g):
    m = 0.9 * m + 0.1 * g
    v = 0.95 * v + 0.05 * g * g
    return bf(w - 0.02 * (m * lax.rsqrt(v + 1e-8) + 0.1 * w)), m, v


def thirds(refs):
    return [refs[n : n + 7] for n in range(0, 21, 7)]


def rows_of(old, big, layer, z, way):
    q = old[0][z].shape[1] // WAYS
    return (layer, pl.ds(way * q, q)), big.at[way // COLOURS, way % COLOURS, :, :, pl.ds((z - 4) * q, q)]


def ahead(arrays, big, layer, ready, sems):
    old, copies = thirds(arrays), []
    for n in range(READY):
        z = 4 + n // WAYS
        where, pieces = rows_of(old, big, layer, z, n % WAYS)
        for s, (src, to) in enumerate(zip([a[z].at[where] for a in old] + [pieces], ready)):
            copies.append(pltpu.make_async_copy(src, to.at[n], sems.at[n, s]))
    return copies


def _update(*refs, layers):
    old, refs = thirds(refs), refs[21:]
    big, small, ready, factor, refs = refs[:layers], refs[layers : 2 * layers], refs[2 * layers : 2 * layers + 4], refs[2 * layers + 4], refs[2 * layers + 5 :]
    new, refs = thirds(refs), refs[21:]
    buffers, (s_in, s_out) = [refs[n : n + 4] for n in range(0, 16, 4)], refs[16:]
    _, d, ff = old[0][4].shape
    q, tall, few = d // WAYS, d // LANES, LANES // WAYS
    f = factor[:1, :1]
    panels = []
    for layer in reversed(range(layers)):
        up = lambda g, i, c: g[c // SIDE, c % SIDE, at(i, TILE), :]
        for n in range(2 * WAYS):
            z = 4 + n // WAYS
            panels.append((0, z, *rows_of(old, big[layer], layer, z, n % WAYS), up))
        for way in range(WAYS):
            def down(g, i, c):
                n, part = lax.div(i, LANES // TILE), lax.rem(i, LANES // TILE)
                w, row = lax.div(part, few // TILE), lax.rem(part, few // TILE)
                return g[lax.div(w, COLOURS), lax.rem(w, COLOURS), n, pl.ds(pl.multiple_of(c * few + row * TILE, TILE), TILE), :]

            panels.append((1, 6, (layer, pl.ds(way * (ff // WAYS), ff // WAYS)), big[layer].at[:, :, way, :, pl.ds(2 * q, q)], down))
        first = 0
        for z in (3, 0, 1, 2):
            count = old[0][z].shape[2] // LANES * tall
            square = lambda g, i, c: g[c * tall + lax.div(i, LANES // TILE), at(lax.rem(i, LANES // TILE), TILE), :]
            panels.append((2 if count > tall else 3, z, (layer,), small[layer].at[pl.ds(first, count)], square))
            first += count
    alike = lambda n, end: sum(panels[m][0] == panels[n][0] for m in range(READY, end))
    order = sorted(range(READY, len(panels)), key=lambda n: (alike(n, n) + 0.5) / alike(n, len(panels)))
    used, jobs = [0] * len(buffers), []
    for kind, z, where, pieces, piece in panels[:READY] + [panels[n] for n in order]:
        slot = used[kind] % buffers[kind][0].shape[0]
        used[kind] += 1
        *held, g = [b.at[slot] for b in buffers[kind]]
        sems = lambda s, n: s.at[kind, slot, n]
        ins, source = [], held
        if len(jobs) < READY:
            *source, g = [r.at[len(jobs)] for r in ready]
        else:
            ins = [pltpu.make_async_copy(src, to, sems(s_in, n)) for n, (src, to) in enumerate(zip([a[z].at[where] for a in old] + [pieces], [*held, g]))]
        outs = [pltpu.make_async_copy(h, a[z].at[where], sems(s_out, n)) for n, (a, h) in enumerate(zip(new, held))]
        jobs.append(((kind, slot), ins, outs, source, held, g, piece))

    def work(source, held, g, piece):
        rows, columns = held[0].shape

        def body(i, _):
            here = at(i, TILE)
            for c in range(columns // LANES):
                part = slice(c * LANES, c * LANES + LANES)
                got = stepped(*(wide(h[here, part]) for h in source), wide(piece(g, i, c)) * f)
                for h, value in zip(held, got):
                    h[here, part] = value
            return _

        lax.fori_loop(0, rows // TILE, body, 0)

    busy, waiting, started = set(), [], set()

    def load(n):
        if n not in started and jobs[n][0] not in busy:
            for copy in jobs[n][1]:
                copy.start()
            busy.add(jobs[n][0])
            started.add(n)

    for n, (slot, ins, outs, source, held, g, piece) in enumerate(jobs):
        for m in range(n, len(jobs)):
            load(m)
        for copy in ins:
            copy.wait()
        work(source, held, g, piece)
        for copy in outs:
            copy.start()
        waiting.append(n)
        for m in waiting[:-1] if n + 1 < len(jobs) else waiting:
            for copy in jobs[m][2]:
                copy.wait()
            busy.discard(jobs[m][0])
        waiting = waiting[-1:]


def update(arrays, big, small, ready, factor):
    layers, d, ff = arrays[4].shape
    kv, q, tall = arrays[1].shape[2], d // WAYS, d // LANES
    small = [s.reshape(-1, LANES, LANES) for s in small]
    given = kept_in(pltpu.HBM, *arrays, *big, *small) + kept_in(pltpu.VMEM, *ready, factor)
    kinds = [(3, (q, ff), (SIDE, SIDE, q, LANES)), (3, (ff // WAYS, d), (CORES, COLOURS, SIDE, q, LANES)), (1, (d, d), (tall * tall, LANES, LANES)), (1, (d, kv), (tall, LANES, LANES))]
    scratch = [vmem(n, *s, dtype=t) for n, panel, pieces in kinds for s, t in ((panel, BF), (panel, F32), (panel, F32), (pieces, BF))]
    return pl.pallas_call(
        functools.partial(_update, layers=layers), name="update", in_specs=[HBM] * (21 + 2 * layers) + [HERE] * 5, out_specs=[ANY] * 21,
        out_shape=[array(*a.shape, dtype=a.dtype) for a in arrays], scratch_shapes=scratch + [semaphores(4, 4, 4), semaphores(4, 4, 3)],
        compiler_params=pltpu.CompilerParams(vmem_limit_bytes=33 * 2**20), cost_estimate=cost(2**28),
    )(*given)


def _finish(pieces, *refs, count, shards):
    shards, arrays, big, refs = refs[:shards], refs[shards : shards + 21], refs[shards + 21], refs[shards + 22 :]
    back, factor, *ready = refs[:6]
    shard, s_ready, *scratch = refs[6:]
    place = Place()
    copies = ahead(arrays, big, arrays[0].shape[0] - 1, ready, s_ready)
    reduce, gather = Reduce(place, pieces, shard, scratch[:8]), Gather(place, shard, back, scratch[8:12])
    pair, line, s_pair, s_line = scratch[12:]
    place.greet()
    reduce.start()
    total = sum(squares(s) for s in shards)
    for copy in copies:
        copy.start()
    for stage in reduce.stages()[1:]:
        stage()
    total = total + squares(shard)
    pair[place.core] = total
    loads = copies
    rounds = [[send(pair.at[place.core], pair.at[place.core], s_pair, (0,), place.partner())]]
    for axis in range(COLOURS):
        mine = line.at[axis, place.places[axis]]
        rounds.append([send(mine, mine, s_line, (axis, far), place.along(axis, far)) for far in FAR])
    gather.start()
    for n, (copies, stage) in enumerate(zip(rounds, (gather.first, gather.relay, gather.second))):
        if n:
            line[n - 1, place.places[n - 1]] = total
        for copy in copies:
            copy.start()
        for copy in copies:
            copy.wait()
        total = sum(line[n - 1, m] for m in range(SIDE)) if n else sum(pair[m] for m in range(CORES))
        stage()
    factor[...] = jnp.broadcast_to(jnp.minimum(ONE, 0.5 * lax.rsqrt(jnp.sum(total, keepdims=True) / count + 1e-30)), factor.shape)
    gather.finish()
    for copy in loads:
        copy.wait()


def finish(pieces, shards, arrays, big, cid, count):
    rows, (_, d, ff) = pieces.shape[-2], arrays[4].shape
    q = d // WAYS
    ready = [pltpu.VMEM((READY, *s), t) for s, t in (((q, ff), BF), ((q, ff), F32), ((q, ff), F32), ((SIDE, SIDE, q, LANES), BF))]
    return pl.pallas_call(
        functools.partial(_finish, count=count, shards=len(shards)), name="finish", in_specs=[ANY] + [HERE] * len(shards) + [HBM] * (len(arrays) + 1),
        out_specs=[HBM] + [HERE] * 5, out_shape=[pltpu.HBM(pieces.shape, BF), pltpu.VMEM((TILE, LANES), F32)] + ready,
        scratch_shapes=[vmem(COLOURS, rows, LANES), semaphores(READY, 4)] + Reduce.scratch(rows) + Gather.scratch(rows)
        + [vmem(CORES, TILE, LANES, dtype=F32), vmem(COLOURS, SIDE, TILE, LANES, dtype=F32), semaphores(2, 1), semaphores(2, COLOURS, SIDE)],
        compiler_params=pltpu.CompilerParams(collective_id=cid, has_side_effects=True, vmem_limit_bytes=20 * 2**20), cost_estimate=cost(2**24),
    )(*kept_in(pltpu.HBM, pieces), *shards, *kept_in(pltpu.HBM, *arrays, big))


def solution(mesh):
    def step(x, dy, *arrays):
        wq, wk, wv, wo, wg, wu, wd = weights = arrays[:7]
        tab = jnp.asarray(rotary(x.shape[1]))
        h, a, q, kv, o, lse, h2, b, silu, slope, act = forward(x[0], tab, *weights)
        kept, mine = (a, q, kv, o, lse, h2, h), (wq, wk, wv, wo, wg, wu)
        cut = lambda g: g.reshape(CORES, COLOURS, SIDE, SIDE, LANES, LANES)
        dg, du, big = gradients(dy[0], silu, slope, b, act, wd, 1, True, None, 0)
        comm = Comm(big, (0, 1, 6, 9, 11, 11, 13, 17, 20, -23))
        dh, small, (s1, big1) = backward(dg, du, dy[0], tab, kept, mine, 1, True, False, comm, 1)
        comm = Comm(cut(small), (0, 1, 2, 3, 4, 4, 6, 7, 8, -9))
        dg, du, big, s2, small1 = gradients(dh, silu, slope, b, act, wd, 0, False, comm, 2)
        comm = Comm(big, (0, 1, 6, 9, 11, 11, 13, 17, -19, -19))
        _, small, (s3, big0) = backward(dg, du, dh, tab, kept, mine, 0, False, True, comm, 3)
        small0, factor, *ready = finish(cut(small), (s1, s2, s3), arrays, big1, 4, sum(w.size for w in weights))
        return tuple(update(arrays, [big0, big1], [small0, small1], ready, factor))

    states, all_of = P(("rep", "dp"), None, None), P(None, None, None)
    return jax.shard_map(step, mesh=mesh, in_specs=(states,) * 2 + (all_of,) * 21, out_specs=(P("rep", None, None),) * 21, check_vma=False)
```

```python
import functools

import jax
import jax.numpy as jnp
import numpy as np
from jax import lax
from jax.experimental import pallas as pl
from jax.experimental.pallas import tpu as pltpu
from jax.sharding import PartitionSpec as P

BF, F32 = jnp.bfloat16, jnp.float32
MESH = pl.DeviceIdType.MESH
HEAD = LANES = 128
HALF = HEAD // 2
THETA = 10000
SIDE = 4
CORES = COLOURS = 2
PIECES = CORES * COLOURS * SIDE * SIDE
WAYS = CORES * COLOURS
TILE = 16
LOG2E = 1.4426950408889634
NEG = -1e30
HIDDEN = NEG + NEG
BLOCK = 512
FINE = 256
AHEAD = 2
PARTS = 2
READY = 6
MEMORY = 63 * 2**20
ONE = 1.0
ANY = pl.BlockSpec(memory_space=pl.ANY)
HERE = pl.BlockSpec(memory_space=pltpu.VMEM)
HBM = pl.BlockSpec(memory_space=pltpu.HBM)


def dot(a, b, ca=1, cb=0):
    return lax.dot_general(a, b, (((ca,), (cb,)), ((), ())), preferred_element_type=F32)


dot_first = functools.partial(dot, ca=0, cb=0)
dot_last = functools.partial(dot, ca=1, cb=1)


def bf(t):
    return t.astype(BF)


def wide(t):
    return t.astype(F32)


def at(n, size):
    return pl.ds(pl.multiple_of(n * size, size), size)


def get(ref):
    return ref[...]


def vmem(*shape, dtype=BF):
    return pltpu.VMEM(shape, dtype)


def array(*shape, dtype=BF):
    return jax.ShapeDtypeStruct(shape, dtype)


def whole(*shape):
    return pl.BlockSpec(shape, lambda i: (0,) * len(shape), pipeline_mode=pl.Buffered(1))


def cols(rows, size, of):
    return pl.BlockSpec((rows, size), lambda i: (0, of(i)))


def tiles(rows, size, of):
    return pl.BlockSpec((None, None, rows, size), lambda i: (*of(i), 0))


def within(i, first, count):
    return jnp.clip(i - first, 0, count - 1)


def mean_square(w):
    return lax.rsqrt(jnp.mean(w * w, 0, keepdims=True) + 1e-6)


def normed(h):
    return bf(wide(h) * mean_square(wide(h)))


def norm_bwd(h, d, dh):
    w, d = wide(h), wide(bf(d))
    r = mean_square(w)
    return bf(wide(dh) + wide(bf(r * (d - w * (r * r * jnp.mean(d * w, 0, keepdims=True))))))


def rotary(tokens):
    angle = np.arange(tokens, dtype=np.float32) * (np.float32(THETA) ** (-np.arange(HALF, dtype=np.float32) / np.float32(HALF)))[:, None]
    return np.concatenate([np.cos(angle), np.sin(angle)]).astype(np.float32)


def turned(t, tab, back=False):
    t = wide(t)
    a, b, c, s = t[:HALF], t[HALF:], tab[:HALF], tab[HALF:]
    s = -s if back else s
    return bf(jnp.concatenate([a * c - b * s, b * c + a * s]))


def gap(ref):
    ref[...] = lax.broadcasted_iota(jnp.int32, ref.shape, 1) - lax.broadcasted_iota(jnp.int32, ref.shape, 0)


def kept_in(space, *arrays):
    return [pltpu.with_memory_space_constraint(a, space) for a in arrays]


class Loads:
    def __init__(self, pairs, sems, first):
        self.copies = [pltpu.make_async_copy(a, b, sems.at[first + n]) for n, (a, b) in enumerate(pairs)]

    def start(self):
        for copy in self.copies:
            copy.start()

    def wait(self):
        for copy in self.copies:
            copy.wait()


def params(collective=None):
    extra = {} if collective is None else dict(collective_id=collective, has_side_effects=True)
    return pltpu.CompilerParams(dimension_semantics=("arbitrary",), vmem_limit_bytes=MEMORY, **extra)


def cost(flops):
    return pl.CostEstimate(flops=flops, transcendentals=0, bytes_accessed=2**25)


def on(step, first, count):
    def run(body):
        pl.when((step >= first) & (step < first + count))(lambda: body(step - first))

    return run


def _forward(x_ref, tab_ref, *refs, layers, heads, blocks, steps):
    wq, wk, wv, wo, wg, wu, wd = refs[:7]
    h_ref, a_ref, q_ref, kv_ref, o_ref, lse_ref, h2_ref, b_ref, silu_ref, slope_ref, act_ref = refs[7:18]
    h_s, q_s, k_s, v_s, o_s, top_s, mix_s, gap_s, b_s, act_s, gate_s, up_s, down_s, wq_s, wk_s, wv_s, wo_s, wg_s, wu_s, wd_s, sems = refs[18:]
    step = pl.program_id(0)
    per = 2 * blocks + steps
    layer, s = lax.div(step, per), lax.rem(step, per)
    early = lambda n: Loads([(w.at[n], t) for w, t in ((wq, wq_s), (wk, wk_s), (wv, wv_s))], sems, 0)
    late = lambda n: Loads([(w.at[n], t) for w, t in ((wo, wo_s), (wg, wg_s), (wu, wu_s), (wd, wd_s))], sems, 3)

    @pl.when(step == 0)
    def _():
        early(layer).start()
        gap(gap_s)
        v_s[HEAD:, :] = jnp.ones_like(v_s[HEAD:, :])

    @pl.when(s == 0)
    def _():
        early(layer).wait()
        late(layer).start()

    @on(s, 0, blocks)
    def _(n):
        here = at(n, BLOCK)

        @pl.when(layer == 0)
        def _():
            h_s[:, here] = get(x_ref).T

        h_ref[...] = h_s[:, here]
        a, tab = normed(h_s[:, here]), get(tab_ref)
        a_ref[...] = a
        q = bf(dot_first(get(wq_s), a))
        for head in range(heads):
            rows = slice(head * HEAD, head * HEAD + HEAD)
            q_s[rows, here] = turned(q[rows], tab)
        q_ref[...] = q_s[:, here]
        k, v = turned(bf(dot_first(get(wk_s), a)), tab), bf(dot_first(get(wv_s), a))
        k_s[here, :] = k.T
        v_s[:HEAD, here] = v
        kv_ref[:HEAD, :], kv_ref[HEAD:, :] = k, v

    @pl.when((s == blocks) & (layer < layers - 1))
    def _():
        early(layer + 1).start()

    @on(s, blocks, blocks)
    def _(n):
        pl.when(n == 0)(late(layer).wait)
        scale = HEAD**-0.5
        e = scale * LOG2E
        top_s[...] = jnp.full(top_s.shape, NEG, F32)
        mix_s[...] = jnp.zeros(mix_s.shape, F32)

        def block(first, size, skip, masked):
            here = pl.ds(pl.multiple_of(first, size), size)
            queries = pl.ds(pl.multiple_of(n * BLOCK + skip, size), BLOCK - skip)
            keys, values = k_s[here, :], v_s[:, here]
            scores = [dot(keys, q_s[head * HEAD : head * HEAD + HEAD, queries]) for head in range(heads)]
            weights, keeps = [], []
            for head, score in enumerate(scores):
                if masked:
                    score = jnp.where(gap_s[:, : BLOCK - skip] >= 0, score, HIDDEN)
                row = slice(head, head + 1)
                old = top_s[row, skip:]
                top = jnp.maximum(old, score.max(axis=0, keepdims=True))
                top_s[row, skip:] = top
                weights.append(bf(jnp.exp2((score - top) * e)))
                keeps.append(jnp.exp2((old - top) * e))
            for head in range(heads):
                mix_s[head, :, skip:] = mix_s[head, :, skip:] * keeps[head] + dot(values, weights[head])

        lax.fori_loop(0, n, lambda j, _: block(j * BLOCK, BLOCK, 0, False), None)
        part = at(n, wg_s.shape[1] // blocks)
        gate_s[part, :], up_s[part, :], down_s[:, part] = wg_s[:, part].T, wu_s[:, part].T, wd_s[part, :].T
        for skip in range(0, BLOCK, FINE):
            block(n * BLOCK + skip, FINE, skip, True)
        for head in range(heads):
            row, rows = slice(head, head + 1), slice(head * HEAD, head * HEAD + HEAD)
            total = mix_s[head, HEAD : HEAD + 1, :]
            o_ref[rows, :] = bf(mix_s[head, :HEAD, :] * (ONE / total))
            lse_ref[row, :] = top_s[row, :] * scale + jnp.log(total)
        o_s[:, at(n, BLOCK)] = get(o_ref)

    @on(s, 2 * blocks, steps)
    def _(n):
        here, part, size = at(lax.div(n, PARTS), BLOCK), lax.rem(n, PARTS), wg_s.shape[1] // PARTS

        @pl.when(part == 0)
        def _():
            h2 = bf(wide(h_s[:, here]) + wide(bf(dot_first(get(wo_s), o_s[:, here]))))
            h_s[:, here], h2_ref[...] = h2, h2
            b = normed(h2)
            b_s[...], b_ref[...] = b, b

        for c in range(0, size, BLOCK):
            mine, all_ = slice(c, c + BLOCK), pl.ds(pl.multiple_of(part * size + c, BLOCK), BLOCK)
            gate, up = dot(gate_s[all_, :], get(b_s)), dot(up_s[all_, :], get(b_s))
            sig = 0.5 * jnp.tanh(0.5 * gate) + 0.5
            silu = gate * sig
            silu_ref[mine, :] = silu
            slope_ref[mine, :] = up * (sig + silu * (ONE - sig))
            act = bf(silu * up)
            act_s[all_, :], act_ref[mine, :] = act, act

        @pl.when((part == PARTS - 1) & (layer < layers - 1))
        def _():
            h_s[:, here] = bf(wide(h_s[:, here]) + wide(bf(dot(get(down_s), get(act_s)))))


def forward(x, tab, wq, wk, wv, wo, wg, wu, wd):
    (t, d), (layers, _, ff) = x.shape, wg.shape
    heads, blocks, steps, kv = d // HEAD, t // BLOCK, t // BLOCK * PARTS, HEAD + HEAD
    per = 2 * blocks + steps
    phase = lambda first, count: lambda i: (lax.div(i, per), within(lax.rem(i, per), first, count))
    qkv, att = phase(0, blocks), phase(blocks, blocks)

    def mlp(i, parts):
        layer, n = phase(2 * blocks, steps)(i)
        return layer, lax.div(n, PARTS), lax.rem(n, parts)

    small, big = lambda rows, of: pl.BlockSpec((None, rows, BLOCK), lambda i: (of(i)[0], 0, of(i)[1])), lambda rows, parts=1: tiles(rows // parts, BLOCK, lambda i: mlp(i, parts))
    make, make_big = lambda rows, dtype=BF: array(layers, rows, t, dtype=dtype), lambda rows, dtype=BF: array(layers, blocks, rows, BLOCK, dtype=dtype)
    return pl.pallas_call(
        functools.partial(_forward, layers=layers, heads=heads, blocks=blocks, steps=steps),
        name="forward",
        grid=(layers * per,),
        in_specs=[pl.BlockSpec((BLOCK, d), lambda i: (within(i, 0, blocks), 0)), cols(HEAD, BLOCK, lambda i: qkv(i)[1])] + [ANY] * 7,
        out_specs=[small(d, qkv), small(d, qkv), small(d, qkv), small(kv, qkv), small(d, att), small(heads, att), big(d), big(d), big(ff, PARTS), big(ff, PARTS), big(ff, PARTS)],
        out_shape=[make(d), make(d), make(d), make(kv), make(d), make(heads, F32), make_big(d), make_big(d), make_big(ff, F32), make_big(ff, F32), make_big(ff)],
        scratch_shapes=[vmem(d, t), vmem(d, t), vmem(t, HEAD), vmem(HEAD + TILE // 2, t), vmem(d, t), vmem(heads, BLOCK, dtype=F32),
                        vmem(heads, HEAD + TILE // 2, BLOCK, dtype=F32), vmem(FINE, BLOCK, dtype=jnp.int32), vmem(d, BLOCK), vmem(ff, BLOCK), vmem(ff, d), vmem(ff, d), vmem(d, ff)]
        + [vmem(*w.shape[1:]) for w in (wq, wk, wv, wo, wg, wu, wd)] + [pltpu.SemaphoreType.DMA((7,))],
        compiler_params=params(),
        cost_estimate=cost(2 * layers * t * d * (d + d + kv + t + 3 * ff)),
    )(x, tab, wq, wk, wv, wo, wg, wu, wd)


FAR = (2, 1, 3)
NEAR = (1, 3)


def halves(up, first):
    return slice(2, SIDE) if up == first else slice(0, 2)


class Place:
    def __init__(self):
        me = lax.axis_index("dp")
        self.core = lax.rem(me, CORES)
        self.places = lax.div(me, SIDE * CORES), lax.rem(lax.div(me, CORES), SIDE)

    def device(self, places, core):
        return {"dp": (places[0] * SIDE + places[1]) * CORES + core}

    def partner(self):
        return self.device(self.places, 1 - self.core)

    def along(self, axis, far):
        return self.device([lax.rem(p + far, SIDE) if n == axis else p for n, p in enumerate(self.places)], self.core)

    def greet(self):
        barrier = pltpu.get_barrier_semaphore()
        peers = [self.partner()] + [self.along(axis, far) for axis in range(COLOURS) for far in FAR]
        for peer in peers:
            pl.semaphore_signal(barrier, inc=1, device_id=peer, device_id_type=MESH)
        pl.semaphore_wait(barrier, len(peers))


def send(src, dst, sems, index, to):
    return pltpu.make_async_remote_copy(src_ref=src, dst_ref=dst, send_sem=sems.at[(0, *index)], recv_sem=sems.at[(1, *index)], device_id=to, device_id_type=MESH)


def add(dst, parts):
    rows = dst.shape[0]
    size = max(n for n in range(TILE, min(FINE, rows) + 1, TILE) if rows % n == 0)

    def body(n, _):
        here = at(n, size)
        dst[here, :] = bf(sum(wide(p[here, :]) for p in parts[1:]) + wide(parts[0][here, :]))
        return _

    lax.fori_loop(0, rows // size, body, 0)


def semaphores(*shape):
    return pltpu.SemaphoreType.DMA(shape)


class Reduce:
    @staticmethod
    def scratch(rows):
        half = vmem(COLOURS, SIDE, SIDE, rows, LANES)
        return [half, half, vmem(COLOURS, SIDE, SIDE, rows, LANES), vmem(COLOURS, SIDE, rows, LANES), semaphores(COLOURS, SIDE),
                semaphores(2, COLOURS, SIDE), semaphores(2, COLOURS, SIDE, 2), semaphores(2, COLOURS, SIDE)]

    def __init__(self, place, pieces, shard, scratch):
        self.place, self.pieces, self.shard = place, pieces, shard
        self.own, self.other, self.one, self.two, self.s_own, self.s_core, self.s_one, self.s_two = scratch
        self.order = [[(far, lax.rem(p + far, SIDE)) for far in (*FAR, 0)] for p in place.places]

    def cores(self, colour, far, n):
        core = self.place.core
        return (send(self.pieces.at[1 - core, colour, n], self.other.at[colour, n], self.s_core, (colour, far), self.place.partner()),
                pltpu.make_async_copy(self.pieces.at[core, colour, n], self.own.at[colour, n], self.s_own.at[colour, far]))

    def near(self, colour, far, first):
        half = halves(far == 1, first)
        n = lax.rem(self.place.places[colour] + far, SIDE)
        return send(self.own.at[colour, n, half], self.one.at[colour, far, half], self.s_one, (colour, far, int(first)), self.place.along(colour, far))

    def across(self, colour, far):
        half = halves(far == 1, False)
        n = lax.rem(self.place.places[colour] + 2, SIDE)
        return send(self.own.at[colour, n, half], self.one.at[colour, 2, half], self.s_one, (colour, 2, int(far == 1)), self.place.along(colour, far))

    def seconds(self, colour, far, n):
        return send(self.own.at[colour, self.place.places[colour], n], self.two.at[colour, far], self.s_two, (colour, far), self.place.along(1 - colour, far))

    def chunks(self, axis_of):
        return [(colour, *self.order[axis_of(colour)][n]) for n in range(SIDE) for colour in range(COLOURS)]

    def start(self):
        for chunk in self.chunks(lambda colour: colour):
            for copy in self.cores(*chunk):
                copy.start()

    def first(self):
        for colour, far, n in self.chunks(lambda colour: colour):
            for copy in self.cores(colour, far, n):
                copy.wait()
            for m in range(SIDE):
                add(self.own.at[colour, n, m], [self.own.at[colour, n, m], self.other.at[colour, n, m]])
            for neighbour in NEAR:
                if far == 2:
                    self.across(colour, neighbour).start()
                if far == neighbour:
                    self.near(colour, far, True).start()

    def relay(self):
        for colour in range(COLOURS):
            for far in NEAR:
                self.across(colour, far).wait()
                n = lax.rem(self.place.places[colour] + far, SIDE)
                for m in range(SIDE)[halves(far == 1, False)]:
                    add(self.own.at[colour, n, m], [self.own.at[colour, n, m], self.one.at[colour, 2, m]])
                self.near(colour, far, False).start()

    def second(self):
        for colour in range(COLOURS):
            for far in NEAR:
                for first in (True, False):
                    self.near(colour, far, first).wait()
        for colour, far, n in self.chunks(lambda colour: 1 - colour):
            mine = self.own.at[colour, self.place.places[colour], n]
            add(mine, [mine] + [self.one.at[colour, f, n] for f in NEAR])
            if far:
                self.seconds(colour, far, n).start()

    def third(self):
        for colour, far, n in self.chunks(lambda colour: 1 - colour):
            if far:
                self.seconds(colour, far, n).wait()
        for colour in range(COLOURS):
            mine = self.own.at[colour, self.place.places[colour], self.place.places[1 - colour]]
            add(self.shard.at[colour], [mine] + [self.two.at[colour, f] for f in FAR])

    def stages(self):
        return [self.start, self.first, self.relay, self.second, self.third]


class Gather:
    @staticmethod
    def scratch(rows):
        return [semaphores(COLOURS), semaphores(2, COLOURS, SIDE), semaphores(2, COLOURS, SIDE, 2), semaphores(2, COLOURS, SIDE)]

    def __init__(self, place, shard, pieces, scratch):
        self.place, self.shard, self.pieces = place, shard, pieces
        self.s_own, self.s_two, self.s_one, self.s_core = scratch

    def place_of(self, colour):
        places = self.place.places
        return self.pieces.at[self.place.core, colour, places[colour], places[1 - colour]]

    def owns(self, colour):
        return pltpu.make_async_copy(self.shard.at[colour], self.place_of(colour), self.s_own.at[colour])

    def seconds(self, colour, far):
        return send(self.shard.at[colour], self.place_of(colour), self.s_two, (colour, far), self.place.along(1 - colour, far))

    def behind(self, colour, far):
        return lax.rem(self.place.places[colour] + SIDE - far, SIDE)

    def near(self, colour, far):
        here = self.pieces.at[self.place.core, colour, self.place.places[colour]]
        return send(here, here, self.s_one, (colour, far, 0), self.place.along(colour, far))

    def across(self, colour, far):
        here = self.pieces.at[self.place.core, colour, self.behind(colour, far), halves(far == 1, True)]
        return send(here, here, self.s_one, (colour, far, 1), self.place.along(colour, far))

    def cores(self, colour, far):
        here = self.pieces.at[self.place.core, colour, self.behind(colour, far)]
        return send(here, here, self.s_core, (colour, far), self.place.partner())

    def start(self):
        for colour in range(COLOURS):
            for far in FAR:
                self.seconds(colour, far).start()
            self.owns(colour).start()

    def first(self):
        for colour in range(COLOURS):
            self.owns(colour).wait()
            for far in FAR:
                self.seconds(colour, far).wait()
            for far in NEAR:
                self.near(colour, far).start()
            self.cores(colour, 0).start()

    def relay(self):
        for colour in range(COLOURS):
            for far in NEAR:
                self.near(colour, far).wait()
                self.across(colour, far).start()
                self.cores(colour, far).start()

    def second(self):
        for colour in range(COLOURS):
            for far in NEAR:
                self.across(colour, far).wait()
            self.cores(colour, 2).start()

    def finish(self):
        for far in (0, *FAR):
            for colour in range(COLOURS):
                self.cores(colour, far).wait()

    def stages(self):
        return [self.start, self.first, self.relay, self.second, self.finish]


class Comm:
    def __init__(self, pieces, points):
        self.pieces, self.points = pieces, points

    def outs(self):
        rows = self.pieces.shape[-2]
        shard = (COLOURS, rows, LANES)
        return ([pl.BlockSpec(shard, lambda i: (0,) * len(shard)), ANY], [array(*shard), array(*self.pieces.shape)], Reduce.scratch(rows) + Gather.scratch(rows))

    def plan(self, pieces, shard, back, *scratch):
        place, n = Place(), len(Reduce.scratch(TILE))
        stages = Reduce(place, pieces, shard, scratch[:n]).stages() + Gather(place, shard, back, scratch[n:]).stages()
        return [(0, place.greet), *zip(self.points, stages, strict=True)]

    def host(self, kernel, opening, n_in, n_out):
        specs, _, scratch = self.outs()

        def body(*refs):
            refs, step = list(refs), pl.program_id(0)
            take = lambda n: [refs.pop(0) for _ in range(n)]
            ins, (pieces,), outs, (shard, back) = take(n_in), take(1), take(n_out), take(len(specs))
            own, found = take(len(refs) - len(scratch)), self.plan(pieces, shard, back, *refs[-len(scratch) :])

            def run(end):
                for point in sorted({p for p, _ in found}):
                    if (point < 0) == end:
                        @pl.when(step == abs(point) - end)
                        def _():
                            for p, stage in found:
                                if p == point:
                                    stage()

            if opening:
                pl.when(step == 0)(lambda: opening(*ins, *outs, *own))
            run(False)
            kernel(*ins, *outs, *own)
            run(True)

        return body


def call(kernel, comm, cid, *, name, grid, in_specs, out_specs, out_shape, scratch_shapes, args, flops, opening=None):
    if comm is not None:
        specs, shapes, scratch = comm.outs()
        kernel = comm.host(kernel, opening, len(in_specs), len(out_specs))
        in_specs, out_specs, out_shape = in_specs + [ANY], out_specs + specs, out_shape + shapes
        scratch_shapes, args = scratch_shapes + scratch, (*args, comm.pieces)
    return pl.pallas_call(kernel, name=name, grid=grid, in_specs=in_specs, out_specs=out_specs, out_shape=out_shape, scratch_shapes=scratch_shapes,
                          compiler_params=params(None if comm is None else cid), cost_estimate=cost(flops))(*args)


def squares(shard):
    def body(n, total):
        here = at(n, TILE)
        return total + sum(wide(shard[colour, here, :]) * wide(shard[colour, here, :]) for colour in range(COLOURS))

    return lax.fori_loop(0, shard.shape[1] // TILE, body, jnp.zeros((TILE, LANES), F32))


def _gradients(dy_ref, silu_ref, slope_ref, b_ref, act_ref, wd_ref, dg_ref, du_ref, grad_ref, gate_s, up_s, down_s, dy_s, stage_s, sems, *, flip, steps):
    n = pl.program_id(0)
    part, size = lax.rem(n, PARTS), silu_ref.shape[0]
    q, few = down_s.shape[0] // WAYS, LANES // WAYS

    def out(part, slot):
        return pltpu.make_async_copy(stage_s.at[slot], grad_ref.at[:, :, part * (size // BLOCK) + slot], sems.at[slot])

    def pieces(slot, z, got):
        got = bf(got).T if z == 2 else bf(got)
        for way in range(WAYS):
            for l in range(SIDE):
                piece, to = stage_s.at[slot, way // COLOURS, way % COLOURS, l], z * q
                if z < 2:
                    piece[to : to + q, :] = got[way * q : way * q + q, l * LANES : l * LANES + LANES]
                else:
                    row = l * LANES + way * few
                    for c in range(0, got.shape[1], LANES):
                        piece[to : to + few, :] = got[row : row + few, c : c + LANES]
                        to += few

    @pl.when(part == 0)
    def _():
        dy_s[...] = dy_ref[...].T if flip else dy_ref[...]

    def work(first, last):
        for slot, c in enumerate(range(0, size, BLOCK)):
            mine, all_ = slice(c, c + BLOCK), pl.ds(pl.multiple_of(part * size + c, BLOCK), BLOCK)
            d = wide(bf(dot(wd_ref[all_, :], get(dy_s))))
            dg_ref[mine, :], du_ref[mine, :] = bf(d * slope_ref[mine, :]), bf(d * silu_ref[mine, :])
            for z, (total, a, other) in enumerate(((gate_s, b_ref, dg_ref), (up_s, b_ref, du_ref), (down_s, dy_s, act_ref))):
                got = dot_last(get(a), other[mine, :])
                got = got if first else total[:, all_] + got
                if last:
                    pieces(slot, z, got)
                else:
                    total[:, all_] = got
            if last:
                out(part, slot).start()

    slots = range(size // BLOCK)

    @pl.when(n == steps - 1)
    def _():
        for slot in slots:
            out(0, slot).wait()

    pl.when(n < PARTS)(lambda: work(True, False))
    pl.when((n >= PARTS) & (n < steps - PARTS))(lambda: work(False, False))
    pl.when(n >= steps - PARTS)(lambda: work(False, True))

    @pl.when(n == steps - 1)
    def _():
        for slot in slots:
            out(part, slot).wait()


def gradients(dy, silu, slope, b, act, wd, layer, flip, comm, cid):
    _, blocks, ff, _ = silu.shape
    d, steps = wd.shape[2], blocks * PARTS
    now, half = lambda i: lax.div(within(i, 0, steps), PARTS), lambda i: lax.rem(within(i, 0, steps), PARTS)
    once = tiles(ff // PARTS, BLOCK, lambda i: (layer, now(i), half(i)))
    mine = pl.BlockSpec((None, ff // PARTS, BLOCK), lambda i: (now(i), half(i), 0))
    grad = (CORES, COLOURS, SIDE, SIDE, 3 * d // WAYS, LANES)
    return call(
        functools.partial(_gradients, flip=flip, steps=steps), comm, cid, name="gradients", grid=(steps,),
        in_specs=[pl.BlockSpec((BLOCK, d), lambda i: (now(i), 0)) if flip else cols(d, BLOCK, now), once, once, tiles(d, BLOCK, lambda i: (layer, now(i), 0)),
                  once, pl.BlockSpec((None, ff, d), lambda i: (layer, 0, 0), pipeline_mode=pl.Buffered(1))],
        out_specs=[mine, mine, ANY],
        out_shape=[array(blocks, ff, BLOCK), array(blocks, ff, BLOCK), array(*grad)],
        scratch_shapes=[vmem(d, ff, dtype=F32)] * 3 + [vmem(d, BLOCK), vmem(ff // PARTS // BLOCK, CORES, COLOURS, SIDE, *grad[-2:]), semaphores(SIDE)],
        args=(dy, silu, slope, b, act, wd), flops=8 * blocks * BLOCK * d * ff,
    )


def _loads(refs, layer):
    a, o, _, wo, wg, wu, wq, wk, wv = refs[10:19]
    *_, a_s, o_s, wo_s, wg_s, wu_s, wq_s, wk_s, wv_s, sems = refs
    pairs = [(r.at[layer], s) for r, s in ((wg, wg_s), (wu, wu_s), (wo, wo_s), (wq, wq_s), (wk, wk_s), (wv, wv_s), (a, a_s), (o, o_s))]
    return Loads(pairs[:3], sems, 0), Loads(pairs[3:], sems, 3)


def _open(*refs, layer):
    for loads in _loads(refs, layer):
        loads.start()


def _backward(*refs, flip, last, heads, steps, blocks, layer):
    first, rest = _loads(refs, layer)
    dg_ref, du_ref, h2_ref, dy_ref, q_ref, kv_ref, o_ref, lse_ref, tab_ref, tabs_ref, _, _, h = refs[:13]
    outs, refs = (refs[19:20], refs[20:]) if last else (refs[19:21], refs[21:])
    dh2_s, do_s, dq_s, dkv_s, k_s, v_s, acc_s, delta_s, dk_s, dv_s, gap_s, db_s, a_s, o_s, wo_s, wg_s, wu_s, wq_s, wk_s, wv_s, _ = refs
    step = pl.program_id(0)
    pairs = blocks * (blocks + 1) // 2
    @pl.when(step == 0)
    def _():
        gap(gap_s)
        k_s[...], v_s[...] = kv_ref[:HEAD, :].T, kv_ref[HEAD:, :].T
        dk_s[...], dv_s[...] = jnp.zeros_like(dk_s), jnp.zeros_like(dv_s)
        first.wait()

    @on(step, 0, steps)
    def _(n):
        here, part = at(lax.div(n, PARTS), BLOCK), at(lax.rem(n, PARTS), dg_ref.shape[0])
        db = dot(wg_s[:, part], get(dg_ref)) + dot(wu_s[:, part], get(du_ref))

        @pl.when(lax.rem(n, PARTS) == 0)
        def _():
            db_s[...] = db

        @pl.when(lax.rem(n, PARTS) > 0)
        def _():
            dh2 = norm_bwd(get(h2_ref), db + get(db_s), get(dy_ref).T if flip else get(dy_ref))
            dh2_s[:, here] = dh2
            do_s[:, here] = bf(dot(get(wo_s), dh2))

    @on(step, steps, pairs)
    def _(n):
        iq = query_block(n, blocks)
        j = n - lax.div(iq * (iq + 1), 2)
        scale = HEAD**-0.5
        e = scale * LOG2E
        mine = at(iq, BLOCK)
        rows = [slice(head * HEAD, head * HEAD + HEAD) for head in range(heads)]

        @pl.when(j == 0)
        def _():
            acc_s[...] = jnp.zeros_like(acc_s)
            for head, r in enumerate(rows):
                delta_s[head : head + 1, :] = (wide(do_s[r, mine]) * wide(o_ref[r, :])).sum(axis=0, keepdims=True)

        def block(start, size, skip, masked):
            here = pl.ds(pl.multiple_of(start, size), size)
            queries = pl.ds(pl.multiple_of(iq * BLOCK + skip, size), BLOCK - skip)
            keys, values, turned_keys = k_s[here, :], v_s[here, :], kv_ref[:HEAD, here]
            qs, dos, pairs_ = [q_ref[r, skip:] for r in rows], [do_s[r, queries] for r in rows], []
            for head in range(heads):
                for n in range(len(pairs_), min(head + AHEAD, heads)):
                    pairs_.append((dot(keys, qs[n]), dot(values, dos[n])))
                score, dp = pairs_[head]
                p = jnp.exp2(score * e - lse_ref[head : head + 1, skip:] * LOG2E)
                if masked:
                    p = jnp.where(gap_s[:, : BLOCK - skip] >= 0, p, 0.0)
                ds = bf(p * (dp - delta_s[head : head + 1, skip:]))
                dv_s[here, :] += dot_last(bf(p), dos[head])
                dk_s[here, :] += dot_last(ds, qs[head])
                acc_s[head, :, skip:] += dot(turned_keys, ds)

        pl.when(j < iq)(lambda: block(j * BLOCK, BLOCK, 0, False))

        @pl.when(j == iq)
        def _():
            for skip in range(0, BLOCK, FINE):
                block(iq * BLOCK + skip, FINE, skip, True)
            for head, r in enumerate(rows):
                dq_s[r, mine] = turned(bf(acc_s[head] * scale), get(tab_ref), True)

        @pl.when(n == pairs - 1)
        def _():
            dkv_s[:HEAD, :] = turned(bf((get(dk_s) * scale).T), get(tabs_ref), True)
            dkv_s[HEAD:, :] = bf(get(dv_s).T)
            rest.wait()

    if not last:
        @on(step, steps + pairs, blocks)
        def _(n):
            here = at(n, BLOCK)
            da = dot(get(wq_s), dq_s[:, here]) + dot(get(wk_s), dkv_s[:HEAD, here]) + dot(get(wv_s), dkv_s[HEAD:, here])
            outs[0][...] = norm_bwd(get(h), da, dh2_s[:, here])

    @pl.when(step == pl.num_programs(0) - 1)
    def _():
        grad_ref, n = outs[-1], 0
        for got in (dot_last(get(o_s), get(dh2_s)), dot_last(get(a_s), get(dq_s)), dot_last(get(a_s), get(dkv_s))):
            for c in range(0, got.shape[1], LANES):
                for r in range(0, got.shape[0], LANES):
                    grad_ref[n] = bf(got[r : r + LANES, c : c + LANES])
                    n += 1
        for n in range(n, PIECES):
            grad_ref[n] = jnp.zeros_like(grad_ref[n])


def query_block(n, blocks):
    return sum(jnp.where(n >= b * (b + 1) // 2, 1, 0) for b in range(1, blocks))


def backward(dg, du, dy, tab, kept, weights, layer, flip, last, comm, cid):
    a, q, kv, o, lse, h2, h = kept
    wq, wk, wv, wo, wg, wu = weights
    (_, d, t), ff = q.shape, dg.shape[1]
    heads, steps, blocks = d // HEAD, t // BLOCK * PARTS, t // BLOCK
    pairs = blocks * (blocks + 1) // 2
    more = 0 if last else blocks
    now, half = lambda i: lax.div(within(i, 0, steps), PARTS), lambda i: lax.rem(within(i, 0, steps), PARTS)
    block = lambda i: query_block(within(i, steps, pairs), blocks)
    then = lambda i: within(i, steps + pairs, blocks)
    hidden = pl.BlockSpec((None, ff // PARTS, BLOCK), lambda i: (now(i), half(i), 0))
    part = lambda rows, of: pl.BlockSpec((None, rows, BLOCK), lambda i: (layer, 0, of(i)))
    out_specs, out_shape = [pl.BlockSpec((PIECES, LANES, LANES), lambda i: (0, 0, 0))], [array(PIECES, LANES, LANES)]
    if not last:
        out_specs, out_shape = [cols(d, BLOCK, then)] + out_specs, [array(d, t)] + out_shape
    got = call(
        functools.partial(_backward, flip=flip, last=last, heads=heads, steps=steps, blocks=blocks, layer=layer), comm, cid, name="backward", opening=functools.partial(_open, layer=layer),
        grid=(steps + pairs + more + 1,),
        in_specs=[hidden, hidden, tiles(d, BLOCK, lambda i: (layer, now(i), 0)), pl.BlockSpec((BLOCK, d), lambda i: (now(i), 0)) if flip else cols(d, BLOCK, now),
                  part(d, block), pl.BlockSpec((None, *kv.shape[1:]), lambda i: (layer, 0, 0), pipeline_mode=pl.Buffered(1)), part(d, block), part(heads, block),
                  cols(HEAD, BLOCK, block), whole(HEAD, t), ANY, ANY, part(d, then)] + [ANY] * 6,
        out_specs=out_specs, out_shape=out_shape,
        scratch_shapes=[vmem(d, t), vmem(d, t), vmem(d, t), vmem(HEAD + HEAD, t), vmem(t, HEAD), vmem(t, HEAD), vmem(heads, HEAD, BLOCK, dtype=F32), vmem(heads, BLOCK, dtype=F32),
                        vmem(t, HEAD, dtype=F32), vmem(t, HEAD, dtype=F32), vmem(FINE, BLOCK, dtype=jnp.int32), vmem(d, BLOCK, dtype=F32), vmem(d, t), vmem(d, t)]
        + [vmem(*w.shape[1:]) for w in (wo, wg, wu, wq, wk, wv)] + [pltpu.SemaphoreType.DMA((8,))],
        args=(dg, du, h2, dy, q, kv, o, lse, tab, tab, a, o, h, wo, wg, wu, wq, wk, wv), flops=4 * t * d * (ff + t + d),
    )
    return (None if last else got[0]), got[0 if last else 1], got[1 if last else 2 :]


def stepped(w, m, v, g):
    m = 0.9 * m + 0.1 * g
    v = 0.95 * v + 0.05 * g * g
    return bf(w - 0.02 * (m * lax.rsqrt(v + 1e-8) + 0.1 * w)), m, v


def thirds(refs):
    return [refs[n : n + 7] for n in range(0, 21, 7)]


def rows_of(old, big, n):
    layer, way = len(big) - 1 - n // (2 * WAYS), n % WAYS
    z = 4 + n // WAYS % 2
    q = old[0][z].shape[1] // WAYS
    return z, (layer, pl.ds(way * q, q)), big[layer].at[way // COLOURS, way % COLOURS, :, :, pl.ds((z - 4) * q, q)]


def ahead(arrays, big, ready, sems):
    old, copies = thirds(arrays), []
    for n in range(READY):
        z, where, pieces = rows_of(old, big, n)
        for s, (src, to) in enumerate(zip([a[z].at[where] for a in old] + [pieces], ready)):
            copies.append(pltpu.make_async_copy(src, to.at[n], sems.at[n, s]))
    return copies


def _update(*refs, layers):
    old, refs = thirds(refs), refs[21:]
    big, small, ready, factor, refs = refs[:layers], refs[layers : 2 * layers], refs[2 * layers : 2 * layers + 4], refs[2 * layers + 4], refs[2 * layers + 5 :]
    new, refs = thirds(refs), refs[21:]
    buffers, (s_in, s_out) = [refs[n : n + 4] for n in range(0, 16, 4)], refs[16:]
    _, d, ff = old[0][4].shape
    q, tall, few = d // WAYS, d // LANES, LANES // WAYS
    f = factor[:1, :1]
    up = lambda g, i, c: g[c // SIDE, c % SIDE, at(i, TILE), :]
    panels = [(0, *rows_of(old, big, n), up) for n in range(2 * WAYS * layers)]
    for layer in range(layers):
        for way in range(WAYS):
            def down(g, i, c):
                n, part = lax.div(i, LANES // TILE), lax.rem(i, LANES // TILE)
                w, row = lax.div(part, few // TILE), lax.rem(part, few // TILE)
                return g[lax.div(w, COLOURS), lax.rem(w, COLOURS), n, pl.ds(pl.multiple_of(c * few + row * TILE, TILE), TILE), :]

            panels.append((1, 6, (layer, pl.ds(way * (ff // WAYS), ff // WAYS)), big[layer].at[:, :, way, :, pl.ds(2 * q, q)], down))
        first = 0
        for z in (3, 0, 1, 2):
            count = old[0][z].shape[2] // LANES * tall
            square = lambda g, i, c: g[c * tall + lax.div(i, LANES // TILE), at(lax.rem(i, LANES // TILE), TILE), :]
            panels.append((2 if count > tall else 3, z, (layer,), small[layer].at[pl.ds(first, count)], square))
            first += count
    alike = lambda n, end: sum(panels[m][0] == panels[n][0] for m in range(READY, end))
    order = sorted(range(READY, len(panels)), key=lambda n: (alike(n, n) + 0.5) / alike(n, len(panels)))
    used, jobs = [0] * len(buffers), []
    for kind, z, where, pieces, piece in panels[:READY] + [panels[n] for n in order]:
        slot = used[kind] % buffers[kind][0].shape[0]
        used[kind] += 1
        *held, g = [b.at[slot] for b in buffers[kind]]
        sems = lambda s, n: s.at[kind, slot, n]
        ins, source = [], held
        if len(jobs) < READY:
            *source, g = [r.at[len(jobs)] for r in ready]
        else:
            ins = [pltpu.make_async_copy(src, to, sems(s_in, n)) for n, (src, to) in enumerate(zip([a[z].at[where] for a in old] + [pieces], [*held, g]))]
        outs = [pltpu.make_async_copy(h, a[z].at[where], sems(s_out, n)) for n, (a, h) in enumerate(zip(new, held))]
        jobs.append(((kind, slot), ins, outs, source, held, g, piece))

    def work(source, held, g, piece):
        rows, columns = held[0].shape

        def body(i, _):
            here = at(i, TILE)
            for c in range(columns // LANES):
                part = slice(c * LANES, c * LANES + LANES)
                got = stepped(*(wide(h[here, part]) for h in source), wide(piece(g, i, c)) * f)
                for h, value in zip(held, got):
                    h[here, part] = value
            return _

        lax.fori_loop(0, rows // TILE, body, 0)

    busy, waiting, started = set(), [], set()

    def load(n):
        if n not in started and jobs[n][0] not in busy:
            for copy in jobs[n][1]:
                copy.start()
            busy.add(jobs[n][0])
            started.add(n)

    for n, (slot, ins, outs, source, held, g, piece) in enumerate(jobs):
        for m in range(n, len(jobs)):
            load(m)
        for copy in ins:
            copy.wait()
        work(source, held, g, piece)
        for copy in outs:
            copy.start()
        waiting.append(n)
        for m in waiting[:-2] if n + 1 < len(jobs) else waiting:
            for copy in jobs[m][2]:
                copy.wait()
            busy.discard(jobs[m][0])
        waiting = waiting[-2:]


def update(arrays, big, small, ready, factor):
    layers, d, ff = arrays[4].shape
    kv, q, tall = arrays[1].shape[2], d // WAYS, d // LANES
    small = [s.reshape(-1, LANES, LANES) for s in small]
    given = kept_in(pltpu.HBM, *arrays, *big, *small) + kept_in(pltpu.VMEM, *ready, factor)
    kinds = [(3, (q, ff), (SIDE, SIDE, q, LANES)), (3, (ff // WAYS, d), (CORES, COLOURS, SIDE, q, LANES)), (1, (d, d), (tall * tall, LANES, LANES)), (1, (d, kv), (tall, LANES, LANES))]
    scratch = [vmem(n, *s, dtype=t) for n, panel, pieces in kinds for s, t in ((panel, BF), (panel, F32), (panel, F32), (pieces, BF))]
    return pl.pallas_call(
        functools.partial(_update, layers=layers), name="update", in_specs=[HBM] * (21 + 2 * layers) + [HERE] * 5, out_specs=[ANY] * 21,
        out_shape=[array(*a.shape, dtype=a.dtype) for a in arrays], scratch_shapes=scratch + [semaphores(4, 4, 4), semaphores(4, 4, 3)],
        compiler_params=pltpu.CompilerParams(vmem_limit_bytes=33 * 2**20), cost_estimate=cost(2**28),
    )(*given)


def _finish(pieces, *refs, count, shards):
    shards, arrays, big, refs = refs[:shards], refs[shards : shards + 21], refs[shards + 21 : shards + 23], refs[shards + 23 :]
    back, factor, *ready = refs[:6]
    shard, s_ready, *scratch = refs[6:]
    place = Place()
    copies = ahead(arrays, big, ready, s_ready)
    *sums, s_sums = scratch[:4]
    scratch, sums = scratch[4:], Loads(list(zip(shards, sums)), s_sums, 0)
    sums.start()
    reduce, gather = Reduce(place, pieces, shard, scratch[:8]), Gather(place, shard, back, scratch[8:12])
    pair, line, s_pair, s_line = scratch[12:]
    place.greet()
    reduce.start()
    sums.wait()
    total = sum(squares(copy.dst_ref) for copy in sums.copies)
    for copy in copies:
        copy.start()
    for stage in reduce.stages()[1:]:
        stage()
    total = total + squares(shard)
    pair[place.core] = total
    loads = copies
    rounds = [[send(pair.at[place.core], pair.at[place.core], s_pair, (0,), place.partner())]]
    for axis in range(COLOURS):
        mine = line.at[axis, place.places[axis]]
        rounds.append([send(mine, mine, s_line, (axis, far), place.along(axis, far)) for far in FAR])
    gather.start()
    for n, (copies, stage) in enumerate(zip(rounds, (gather.first, gather.relay, gather.second))):
        if n:
            line[n - 1, place.places[n - 1]] = total
        for copy in copies:
            copy.start()
        for copy in copies:
            copy.wait()
        total = sum(line[n - 1, m] for m in range(SIDE)) if n else sum(pair[m] for m in range(CORES))
        stage()
    factor[...] = jnp.broadcast_to(jnp.minimum(ONE, 0.5 * lax.rsqrt(jnp.sum(total, keepdims=True) / count + 1e-30)), factor.shape)
    gather.finish()
    for copy in loads:
        copy.wait()


def finish(pieces, shards, arrays, big, cid, count):
    rows, (_, d, ff) = pieces.shape[-2], arrays[4].shape
    q = d // WAYS
    ready = [pltpu.VMEM((READY, *s), t) for s, t in (((q, ff), BF), ((q, ff), F32), ((q, ff), F32), ((SIDE, SIDE, q, LANES), BF))]
    return pl.pallas_call(
        functools.partial(_finish, count=count, shards=len(shards)), name="finish", in_specs=[HBM] * (1 + len(shards) + len(arrays) + len(big)),
        out_specs=[HBM] + [HERE] * 5, out_shape=[pltpu.HBM(pieces.shape, BF), pltpu.VMEM((TILE, LANES), F32)] + ready,
        scratch_shapes=[vmem(COLOURS, rows, LANES), semaphores(READY, 4)] + [vmem(*s.shape) for s in shards] + [semaphores(len(shards))] + Reduce.scratch(rows) + Gather.scratch(rows)
        + [vmem(CORES, TILE, LANES, dtype=F32), vmem(COLOURS, SIDE, TILE, LANES, dtype=F32), semaphores(2, 1), semaphores(2, COLOURS, SIDE)],
        compiler_params=pltpu.CompilerParams(collective_id=cid, has_side_effects=True, vmem_limit_bytes=20 * 2**20), cost_estimate=cost(2**24),
    )(*kept_in(pltpu.HBM, pieces, *shards, *arrays, *big))


def solution(mesh):
    def step(x, dy, *arrays):
        wq, wk, wv, wo, wg, wu, wd = weights = arrays[:7]
        tab = jnp.asarray(rotary(x.shape[1]))
        h, a, q, kv, o, lse, h2, b, silu, slope, act = forward(x[0], tab, *weights)
        kept, mine = (a, q, kv, o, lse, h2, h), (wq, wk, wv, wo, wg, wu)
        cut = lambda g: g.reshape(CORES, COLOURS, SIDE, SIDE, LANES, LANES)
        dg, du, big = gradients(dy[0], silu, slope, b, act, wd, 1, True, None, 0)
        comm = Comm(big, (0, 1, 6, 9, 11, 11, 13, 17, 20, -23))
        dh, small, (s1, big1) = backward(dg, du, dy[0], tab, kept, mine, 1, True, False, comm, 1)
        comm = Comm(cut(small), (0, 1, 2, 3, 4, 4, 5, 6, 7, -8))
        dg, du, big, s2, small1 = gradients(dh, silu, slope, b, act, wd, 0, False, comm, 2)
        comm = Comm(big, (0, 1, 6, 9, 11, 11, 13, 17, -19, -19))
        _, small, (s3, big0) = backward(dg, du, dh, tab, kept, mine, 0, False, True, comm, 3)
        small0, factor, *ready = finish(cut(small), (s1, s2, s3), arrays, (big0, big1), 4, sum(w.size for w in weights))
        return tuple(update(arrays, [big0, big1], [small0, small1], ready, factor))

    states, all_of = P(("rep", "dp"), None, None), P(None, None, None)
    return jax.shard_map(step, mesh=mesh, in_specs=(states,) * 2 + (all_of,) * 21, out_specs=(P("rep", None, None),) * 21, check_vma=False)
```

```python
import functools

import jax
import jax.numpy as jnp
import numpy as np
from jax import lax
from jax.experimental import pallas as pl
from jax.experimental.pallas import tpu as pltpu
from jax.sharding import PartitionSpec as P

BF, F32 = jnp.bfloat16, jnp.float32
MESH = pl.DeviceIdType.MESH
HEAD = LANES = 128
HALF = HEAD // 2
THETA = 10000
SIDE = 4
CORES = COLOURS = 2
PIECES = CORES * COLOURS * SIDE * SIDE
WAYS = CORES * COLOURS
TILE = 16
LOG2E = 1.4426950408889634
NEG = -1e30
HIDDEN = NEG + NEG
BLOCK = 512
FINE = 256
AHEAD = 2
PARTS = 2
READY = 6
MEMORY = 63 * 2**20
ONE = 1.0
ANY = pl.BlockSpec(memory_space=pl.ANY)
HERE = pl.BlockSpec(memory_space=pltpu.VMEM)
HBM = pl.BlockSpec(memory_space=pltpu.HBM)


def dot(a, b, ca=1, cb=0):
    return lax.dot_general(a, b, (((ca,), (cb,)), ((), ())), preferred_element_type=F32)


dot_first = functools.partial(dot, ca=0, cb=0)
dot_last = functools.partial(dot, ca=1, cb=1)


def bf(t):
    return t.astype(BF)


def wide(t):
    return t.astype(F32)


def at(n, size):
    return pl.ds(pl.multiple_of(n * size, size), size)


def get(ref):
    return ref[...]


def vmem(*shape, dtype=BF):
    return pltpu.VMEM(shape, dtype)


def array(*shape, dtype=BF):
    return jax.ShapeDtypeStruct(shape, dtype)


def whole(*shape):
    return pl.BlockSpec(shape, lambda i: (0,) * len(shape), pipeline_mode=pl.Buffered(1))


def cols(rows, size, of):
    return pl.BlockSpec((rows, size), lambda i: (0, of(i)))


def tiles(rows, size, of):
    return pl.BlockSpec((None, None, rows, size), lambda i: (*of(i), 0))


def within(i, first, count):
    return jnp.clip(i - first, 0, count - 1)


def mean_square(w):
    return lax.rsqrt(jnp.mean(w * w, 0, keepdims=True) + 1e-6)


def normed(h):
    return bf(wide(h) * mean_square(wide(h)))


def norm_bwd(h, d, dh):
    w, d = wide(h), wide(bf(d))
    r = mean_square(w)
    return bf(wide(dh) + wide(bf(r * (d - w * (r * r * jnp.mean(d * w, 0, keepdims=True))))))


def rotary(tokens):
    angle = np.arange(tokens, dtype=np.float32) * (np.float32(THETA) ** (-np.arange(HALF, dtype=np.float32) / np.float32(HALF)))[:, None]
    return np.concatenate([np.cos(angle), np.sin(angle)]).astype(np.float32)


def turned(t, tab, back=False):
    t = wide(t)
    a, b, c, s = t[:HALF], t[HALF:], tab[:HALF], tab[HALF:]
    s = -s if back else s
    return bf(jnp.concatenate([a * c - b * s, b * c + a * s]))


def gap(ref):
    ref[...] = lax.broadcasted_iota(jnp.int32, ref.shape, 1) - lax.broadcasted_iota(jnp.int32, ref.shape, 0)


def kept_in(space, *arrays):
    return [pltpu.with_memory_space_constraint(a, space) for a in arrays]


class Loads:
    def __init__(self, pairs, sems, first):
        self.copies = [pltpu.make_async_copy(a, b, sems.at[first + n]) for n, (a, b) in enumerate(pairs)]

    def start(self):
        for copy in self.copies:
            copy.start()

    def wait(self):
        for copy in self.copies:
            copy.wait()


def params(collective=None):
    extra = {} if collective is None else dict(collective_id=collective, has_side_effects=True)
    return pltpu.CompilerParams(dimension_semantics=("arbitrary",), vmem_limit_bytes=MEMORY, **extra)


def cost(flops):
    return pl.CostEstimate(flops=flops, transcendentals=0, bytes_accessed=2**25)


def on(step, first, count):
    def run(body):
        pl.when((step >= first) & (step < first + count))(lambda: body(step - first))

    return run


def _forward(x_ref, tab_ref, *refs, layers, heads, blocks, steps):
    wq, wk, wv, wo, wg, wu, wd = refs[:7]
    h_ref, a_ref, q_ref, kv_ref, o_ref, lse_ref, h2_ref, b_ref, silu_ref, slope_ref, act_ref = refs[7:18]
    h_s, q_s, k_s, v_s, o_s, top_s, mix_s, gap_s, b_s, act_s, gate_s, up_s, down_s, wq_s, wk_s, wv_s, wo_s, wg_s, wu_s, wd_s, sems = refs[18:]
    step = pl.program_id(0)
    per = 2 * blocks + steps
    layer, s = lax.div(step, per), lax.rem(step, per)
    early = lambda n: Loads([(w.at[n], t) for w, t in ((wq, wq_s), (wk, wk_s), (wv, wv_s))], sems, 0)
    late = lambda n: Loads([(w.at[n], t) for w, t in ((wo, wo_s), (wg, wg_s), (wu, wu_s), (wd, wd_s))], sems, 3)

    @pl.when(step == 0)
    def _():
        early(layer).start()
        gap(gap_s)
        v_s[HEAD:, :] = jnp.ones_like(v_s[HEAD:, :])

    @pl.when(s == 0)
    def _():
        early(layer).wait()
        late(layer).start()

    @on(s, 0, blocks)
    def _(n):
        here = at(n, BLOCK)

        @pl.when(layer == 0)
        def _():
            h_s[:, here] = get(x_ref).T

        h_ref[...] = h_s[:, here]
        a, tab = normed(h_s[:, here]), get(tab_ref)
        a_ref[...] = a
        q = bf(dot_first(get(wq_s), a))
        for head in range(heads):
            rows = slice(head * HEAD, head * HEAD + HEAD)
            q_s[rows, here] = turned(q[rows], tab)
        q_ref[...] = q_s[:, here]
        k, v = turned(bf(dot_first(get(wk_s), a)), tab), bf(dot_first(get(wv_s), a))
        k_s[here, :] = k.T
        v_s[:HEAD, here] = v
        kv_ref[:HEAD, :], kv_ref[HEAD:, :] = k, v

    @pl.when((s == blocks) & (layer < layers - 1))
    def _():
        early(layer + 1).start()

    @on(s, blocks, blocks)
    def _(n):
        pl.when(n == 0)(late(layer).wait)
        scale = HEAD**-0.5
        e = scale * LOG2E
        top_s[...] = jnp.full(top_s.shape, NEG, F32)
        mix_s[...] = jnp.zeros(mix_s.shape, F32)

        def block(first, size, skip, masked):
            here = pl.ds(pl.multiple_of(first, size), size)
            queries = pl.ds(pl.multiple_of(n * BLOCK + skip, size), BLOCK - skip)
            keys, values = k_s[here, :], v_s[:, here]
            scores = [dot(keys, q_s[head * HEAD : head * HEAD + HEAD, queries]) for head in range(heads)]
            weights, keeps = [], []
            for head, score in enumerate(scores):
                if masked:
                    score = jnp.where(gap_s[:, : BLOCK - skip] >= 0, score, HIDDEN)
                row = slice(head, head + 1)
                old = top_s[row, skip:]
                top = jnp.maximum(old, score.max(axis=0, keepdims=True))
                top_s[row, skip:] = top
                weights.append(bf(jnp.exp2((score - top) * e)))
                keeps.append(jnp.exp2((old - top) * e))
            for head in range(heads):
                mix_s[head, :, skip:] = mix_s[head, :, skip:] * keeps[head] + dot(values, weights[head])

        lax.fori_loop(0, n, lambda j, _: block(j * BLOCK, BLOCK, 0, False), None)
        part = at(n, wg_s.shape[1] // blocks)
        gate_s[part, :], up_s[part, :], down_s[:, part] = wg_s[:, part].T, wu_s[:, part].T, wd_s[part, :].T
        for skip in range(0, BLOCK, FINE):
            block(n * BLOCK + skip, FINE, skip, True)
        for head in range(heads):
            row, rows = slice(head, head + 1), slice(head * HEAD, head * HEAD + HEAD)
            total = mix_s[head, HEAD : HEAD + 1, :]
            o_ref[rows, :] = bf(mix_s[head, :HEAD, :] * (ONE / total))
            lse_ref[row, :] = top_s[row, :] * scale + jnp.log(total)
        o_s[:, at(n, BLOCK)] = get(o_ref)

    @on(s, 2 * blocks, steps)
    def _(n):
        here, part, size = at(lax.div(n, PARTS), BLOCK), lax.rem(n, PARTS), wg_s.shape[1] // PARTS

        @pl.when(part == 0)
        def _():
            h2 = bf(wide(h_s[:, here]) + wide(bf(dot_first(get(wo_s), o_s[:, here]))))
            h_s[:, here], h2_ref[...] = h2, h2
            b = normed(h2)
            b_s[...], b_ref[...] = b, b

        for c in range(0, size, BLOCK):
            mine, all_ = slice(c, c + BLOCK), pl.ds(pl.multiple_of(part * size + c, BLOCK), BLOCK)
            gate, up = dot(gate_s[all_, :], get(b_s)), dot(up_s[all_, :], get(b_s))
            sig = 0.5 * jnp.tanh(0.5 * gate) + 0.5
            silu = gate * sig
            silu_ref[mine, :] = silu
            slope_ref[mine, :] = up * (sig + silu * (ONE - sig))
            act = bf(silu * up)
            act_s[all_, :], act_ref[mine, :] = act, act

        @pl.when((part == PARTS - 1) & (layer < layers - 1))
        def _():
            h_s[:, here] = bf(wide(h_s[:, here]) + wide(bf(dot(get(down_s), get(act_s)))))


def forward(x, tab, wq, wk, wv, wo, wg, wu, wd):
    (t, d), (layers, _, ff) = x.shape, wg.shape
    heads, blocks, steps, kv = d // HEAD, t // BLOCK, t // BLOCK * PARTS, HEAD + HEAD
    per = 2 * blocks + steps
    phase = lambda first, count: lambda i: (lax.div(i, per), within(lax.rem(i, per), first, count))
    qkv, att = phase(0, blocks), phase(blocks, blocks)

    def mlp(i, parts):
        layer, n = phase(2 * blocks, steps)(i)
        return layer, lax.div(n, PARTS), lax.rem(n, parts)

    small, big = lambda rows, of: pl.BlockSpec((None, rows, BLOCK), lambda i: (of(i)[0], 0, of(i)[1])), lambda rows, parts=1: tiles(rows // parts, BLOCK, lambda i: mlp(i, parts))
    make, make_big = lambda rows, dtype=BF: array(layers, rows, t, dtype=dtype), lambda rows, dtype=BF: array(layers, blocks, rows, BLOCK, dtype=dtype)
    return pl.pallas_call(
        functools.partial(_forward, layers=layers, heads=heads, blocks=blocks, steps=steps),
        name="forward",
        grid=(layers * per,),
        in_specs=[pl.BlockSpec((BLOCK, d), lambda i: (within(i, 0, blocks), 0)), cols(HEAD, BLOCK, lambda i: qkv(i)[1])] + [ANY] * 7,
        out_specs=[small(d, qkv), small(d, qkv), small(d, qkv), small(kv, qkv), small(d, att), small(heads, att), big(d), big(d), big(ff, PARTS), big(ff, PARTS), big(ff, PARTS)],
        out_shape=[make(d), make(d), make(d), make(kv), make(d), make(heads, F32), make_big(d), make_big(d), make_big(ff, F32), make_big(ff, F32), make_big(ff)],
        scratch_shapes=[vmem(d, t), vmem(d, t), vmem(t, HEAD), vmem(HEAD + TILE // 2, t), vmem(d, t), vmem(heads, BLOCK, dtype=F32),
                        vmem(heads, HEAD + TILE // 2, BLOCK, dtype=F32), vmem(FINE, BLOCK, dtype=jnp.int32), vmem(d, BLOCK), vmem(ff, BLOCK), vmem(ff, d), vmem(ff, d), vmem(d, ff)]
        + [vmem(*w.shape[1:]) for w in (wq, wk, wv, wo, wg, wu, wd)] + [pltpu.SemaphoreType.DMA((7,))],
        compiler_params=params(),
        cost_estimate=cost(2 * layers * t * d * (d + d + kv + t + 3 * ff)),
    )(x, tab, wq, wk, wv, wo, wg, wu, wd)


FAR = (2, 1, 3)
NEAR = (1, 3)


def halves(up, first):
    return slice(2, SIDE) if up == first else slice(0, 2)


class Place:
    def __init__(self):
        me = lax.axis_index("dp")
        self.core = lax.rem(me, CORES)
        self.places = lax.div(me, SIDE * CORES), lax.rem(lax.div(me, CORES), SIDE)

    def device(self, places, core):
        return {"dp": (places[0] * SIDE + places[1]) * CORES + core}

    def partner(self):
        return self.device(self.places, 1 - self.core)

    def along(self, axis, far):
        return self.device([lax.rem(p + far, SIDE) if n == axis else p for n, p in enumerate(self.places)], self.core)

    def greet(self):
        barrier = pltpu.get_barrier_semaphore()
        peers = [self.partner()] + [self.along(axis, far) for axis in range(COLOURS) for far in FAR]
        for peer in peers:
            pl.semaphore_signal(barrier, inc=1, device_id=peer, device_id_type=MESH)
        pl.semaphore_wait(barrier, len(peers))


def send(src, dst, sems, index, to):
    return pltpu.make_async_remote_copy(src_ref=src, dst_ref=dst, send_sem=sems.at[(0, *index)], recv_sem=sems.at[(1, *index)], device_id=to, device_id_type=MESH)


def add(dst, parts):
    rows = dst.shape[0]
    size = max(n for n in range(TILE, min(FINE, rows) + 1, TILE) if rows % n == 0)

    def body(n, _):
        here = at(n, size)
        dst[here, :] = bf(sum(wide(p[here, :]) for p in parts[1:]) + wide(parts[0][here, :]))
        return _

    lax.fori_loop(0, rows // size, body, 0)


def semaphores(*shape):
    return pltpu.SemaphoreType.DMA(shape)


class Reduce:
    @staticmethod
    def scratch(rows):
        half = vmem(COLOURS, SIDE, SIDE, rows, LANES)
        return [half, half, vmem(COLOURS, SIDE, SIDE, rows, LANES), vmem(COLOURS, SIDE, rows, LANES), semaphores(COLOURS, SIDE),
                semaphores(2, COLOURS, SIDE), semaphores(2, COLOURS, SIDE, 2), semaphores(2, COLOURS, SIDE)]

    def __init__(self, place, pieces, shard, scratch):
        self.place, self.pieces, self.shard = place, pieces, shard
        self.own, self.other, self.one, self.two, self.s_own, self.s_core, self.s_one, self.s_two = scratch
        self.order = [[(far, lax.rem(p + far, SIDE)) for far in (*FAR, 0)] for p in place.places]

    def cores(self, colour, far, n):
        core = self.place.core
        return (send(self.pieces.at[1 - core, colour, n], self.other.at[colour, n], self.s_core, (colour, far), self.place.partner()),
                pltpu.make_async_copy(self.pieces.at[core, colour, n], self.own.at[colour, n], self.s_own.at[colour, far]))

    def near(self, colour, far, first):
        half = halves(far == 1, first)
        n = lax.rem(self.place.places[colour] + far, SIDE)
        return send(self.own.at[colour, n, half], self.one.at[colour, far, half], self.s_one, (colour, far, int(first)), self.place.along(colour, far))

    def across(self, colour, far):
        half = halves(far == 1, False)
        n = lax.rem(self.place.places[colour] + 2, SIDE)
        return send(self.own.at[colour, n, half], self.one.at[colour, 2, half], self.s_one, (colour, 2, int(far == 1)), self.place.along(colour, far))

    def seconds(self, colour, far, n):
        return send(self.own.at[colour, self.place.places[colour], n], self.two.at[colour, far], self.s_two, (colour, far), self.place.along(1 - colour, far))

    def chunks(self, axis_of):
        return [(colour, *self.order[axis_of(colour)][n]) for n in range(SIDE) for colour in range(COLOURS)]

    def start(self):
        for chunk in self.chunks(lambda colour: colour):
            for copy in self.cores(*chunk):
                copy.start()

    def first(self):
        for colour, far, n in self.chunks(lambda colour: colour):
            for copy in self.cores(colour, far, n):
                copy.wait()
            now = slice(SIDE) if far == 2 else halves(far == 1, True) if far else slice(0)
            for m in range(SIDE)[now]:
                add(self.own.at[colour, n, m], [self.own.at[colour, n, m], self.other.at[colour, n, m]])
            for neighbour in NEAR:
                if far == 2:
                    self.across(colour, neighbour).start()
                if far == neighbour:
                    self.near(colour, far, True).start()

    def relay(self):
        for colour in range(COLOURS):
            for far in NEAR:
                self.across(colour, far).wait()
                n = lax.rem(self.place.places[colour] + far, SIDE)
                for m in range(SIDE)[halves(far == 1, False)]:
                    add(self.own.at[colour, n, m], [self.own.at[colour, n, m], self.other.at[colour, n, m], self.one.at[colour, 2, m]])
                self.near(colour, far, False).start()

    def second(self):
        for colour in range(COLOURS):
            for far in NEAR:
                for first in (True, False):
                    self.near(colour, far, first).wait()
        for colour, far, n in self.chunks(lambda colour: 1 - colour):
            place = self.place.places[colour]
            mine = self.own.at[colour, place, n]
            add(mine, [mine, self.other.at[colour, place, n]] + [self.one.at[colour, f, n] for f in NEAR])
            if far:
                self.seconds(colour, far, n).start()

    def third(self):
        for colour, far, n in self.chunks(lambda colour: 1 - colour):
            if far:
                self.seconds(colour, far, n).wait()
        for colour in range(COLOURS):
            mine = self.own.at[colour, self.place.places[colour], self.place.places[1 - colour]]
            add(self.shard.at[colour], [mine] + [self.two.at[colour, f] for f in FAR])

    def stages(self):
        return [self.start, self.first, self.relay, self.second, self.third]


class Gather:
    @staticmethod
    def scratch(rows):
        return [semaphores(COLOURS), semaphores(2, COLOURS, SIDE), semaphores(2, COLOURS, SIDE, 2), semaphores(2, COLOURS, SIDE)]

    def __init__(self, place, shard, pieces, scratch):
        self.place, self.shard, self.pieces = place, shard, pieces
        self.s_own, self.s_two, self.s_one, self.s_core = scratch

    def place_of(self, colour):
        places = self.place.places
        return self.pieces.at[self.place.core, colour, places[colour], places[1 - colour]]

    def owns(self, colour):
        return pltpu.make_async_copy(self.shard.at[colour], self.place_of(colour), self.s_own.at[colour])

    def seconds(self, colour, far):
        return send(self.shard.at[colour], self.place_of(colour), self.s_two, (colour, far), self.place.along(1 - colour, far))

    def behind(self, colour, far):
        return lax.rem(self.place.places[colour] + SIDE - far, SIDE)

    def near(self, colour, far):
        here = self.pieces.at[self.place.core, colour, self.place.places[colour]]
        return send(here, here, self.s_one, (colour, far, 0), self.place.along(colour, far))

    def across(self, colour, far):
        here = self.pieces.at[self.place.core, colour, self.behind(colour, far), halves(far == 1, True)]
        return send(here, here, self.s_one, (colour, far, 1), self.place.along(colour, far))

    def cores(self, colour, far):
        here = self.pieces.at[self.place.core, colour, self.behind(colour, far)]
        return send(here, here, self.s_core, (colour, far), self.place.partner())

    def start(self):
        for colour in range(COLOURS):
            for far in FAR:
                self.seconds(colour, far).start()
            self.owns(colour).start()

    def first(self):
        for colour in range(COLOURS):
            self.owns(colour).wait()
            for far in FAR:
                self.seconds(colour, far).wait()
            for far in NEAR:
                self.near(colour, far).start()
            self.cores(colour, 0).start()

    def relay(self):
        for colour in range(COLOURS):
            for far in NEAR:
                self.near(colour, far).wait()
                self.across(colour, far).start()
                self.cores(colour, far).start()

    def second(self):
        for colour in range(COLOURS):
            for far in NEAR:
                self.across(colour, far).wait()
            self.cores(colour, 2).start()

    def finish(self):
        for far in (0, *FAR):
            for colour in range(COLOURS):
                self.cores(colour, far).wait()

    def stages(self):
        return [self.start, self.first, self.relay, self.second, self.finish]


class Comm:
    def __init__(self, pieces, points):
        self.pieces, self.points = pieces, points

    def outs(self):
        rows = self.pieces.shape[-2]
        shard = (COLOURS, rows, LANES)
        return ([pl.BlockSpec(shard, lambda i: (0,) * len(shard)), ANY], [array(*shard), array(*self.pieces.shape)], Reduce.scratch(rows) + Gather.scratch(rows))

    def plan(self, pieces, shard, back, *scratch):
        place, n = Place(), len(Reduce.scratch(TILE))
        stages = Reduce(place, pieces, shard, scratch[:n]).stages() + Gather(place, shard, back, scratch[n:]).stages()
        return [(0, place.greet), *zip(self.points, stages, strict=True)]

    def host(self, kernel, opening, n_in, n_out):
        specs, _, scratch = self.outs()

        def body(*refs):
            refs, step = list(refs), pl.program_id(0)
            take = lambda n: [refs.pop(0) for _ in range(n)]
            ins, (pieces,), outs, (shard, back) = take(n_in), take(1), take(n_out), take(len(specs))
            own, found = take(len(refs) - len(scratch)), self.plan(pieces, shard, back, *refs[-len(scratch) :])

            def run(end):
                for point in sorted({p for p, _ in found}):
                    if (point < 0) == end:
                        @pl.when(step == abs(point) - end)
                        def _():
                            for p, stage in found:
                                if p == point:
                                    stage()

            if opening:
                pl.when(step == 0)(lambda: opening(*ins, *outs, *own))
            run(False)
            kernel(*ins, *outs, *own)
            run(True)

        return body


def call(kernel, comm, cid, *, name, grid, in_specs, out_specs, out_shape, scratch_shapes, args, flops, opening=None):
    if comm is not None:
        specs, shapes, scratch = comm.outs()
        kernel = comm.host(kernel, opening, len(in_specs), len(out_specs))
        in_specs, out_specs, out_shape = in_specs + [ANY], out_specs + specs, out_shape + shapes
        scratch_shapes, args = scratch_shapes + scratch, (*args, comm.pieces)
    return pl.pallas_call(kernel, name=name, grid=grid, in_specs=in_specs, out_specs=out_specs, out_shape=out_shape, scratch_shapes=scratch_shapes,
                          compiler_params=params(None if comm is None else cid), cost_estimate=cost(flops))(*args)


def squares(shard):
    def body(n, total):
        here = at(n, TILE)
        return total + sum(wide(shard[colour, here, :]) * wide(shard[colour, here, :]) for colour in range(COLOURS))

    return lax.fori_loop(0, shard.shape[1] // TILE, body, jnp.zeros((TILE, LANES), F32))


def _gradients(dy_ref, silu_ref, slope_ref, b_ref, act_ref, wd_ref, dg_ref, du_ref, grad_ref, gate_s, up_s, down_s, dy_s, stage_s, sems, *, flip, steps):
    n = pl.program_id(0)
    part, size = lax.rem(n, PARTS), silu_ref.shape[0]
    q, few = down_s.shape[0] // WAYS, LANES // WAYS

    def out(part, slot):
        return pltpu.make_async_copy(stage_s.at[slot], grad_ref.at[:, :, part * (size // BLOCK) + slot], sems.at[slot])

    def pieces(slot, z, got):
        got = bf(got).T if z == 2 else bf(got)
        for way in range(WAYS):
            for l in range(SIDE):
                piece, to = stage_s.at[slot, way // COLOURS, way % COLOURS, l], z * q
                if z < 2:
                    piece[to : to + q, :] = got[way * q : way * q + q, l * LANES : l * LANES + LANES]
                else:
                    row = l * LANES + way * few
                    for c in range(0, got.shape[1], LANES):
                        piece[to : to + few, :] = got[row : row + few, c : c + LANES]
                        to += few

    @pl.when(part == 0)
    def _():
        dy_s[...] = dy_ref[...].T if flip else dy_ref[...]

    def work(first, last):
        for slot, c in enumerate(range(0, size, BLOCK)):
            mine, all_ = slice(c, c + BLOCK), pl.ds(pl.multiple_of(part * size + c, BLOCK), BLOCK)
            d = wide(bf(dot(wd_ref[all_, :], get(dy_s))))
            dg_ref[mine, :], du_ref[mine, :] = bf(d * slope_ref[mine, :]), bf(d * silu_ref[mine, :])
            for z, (total, a, other) in enumerate(((gate_s, b_ref, dg_ref), (up_s, b_ref, du_ref), (down_s, dy_s, act_ref))):
                got = dot_last(get(a), other[mine, :])
                got = got if first else total[:, all_] + got
                if last:
                    pieces(slot, z, got)
                else:
                    total[:, all_] = got
            if last:
                out(part, slot).start()

    slots = range(size // BLOCK)

    @pl.when(n == steps - 1)
    def _():
        for slot in slots:
            out(0, slot).wait()

    pl.when(n < PARTS)(lambda: work(True, False))
    pl.when((n >= PARTS) & (n < steps - PARTS))(lambda: work(False, False))
    pl.when(n >= steps - PARTS)(lambda: work(False, True))

    @pl.when(n == steps - 1)
    def _():
        for slot in slots:
            out(part, slot).wait()


def gradients(dy, silu, slope, b, act, wd, layer, flip, comm, cid):
    _, blocks, ff, _ = silu.shape
    d, steps = wd.shape[2], blocks * PARTS
    now, half = lambda i: lax.div(within(i, 0, steps), PARTS), lambda i: lax.rem(within(i, 0, steps), PARTS)
    once = tiles(ff // PARTS, BLOCK, lambda i: (layer, now(i), half(i)))
    mine = pl.BlockSpec((None, ff // PARTS, BLOCK), lambda i: (now(i), half(i), 0))
    grad = (CORES, COLOURS, SIDE, SIDE, 3 * d // WAYS, LANES)
    return call(
        functools.partial(_gradients, flip=flip, steps=steps), comm, cid, name="gradients", grid=(steps,),
        in_specs=[pl.BlockSpec((BLOCK, d), lambda i: (now(i), 0)) if flip else cols(d, BLOCK, now), once, once, tiles(d, BLOCK, lambda i: (layer, now(i), 0)),
                  once, pl.BlockSpec((None, ff, d), lambda i: (layer, 0, 0), pipeline_mode=pl.Buffered(1))],
        out_specs=[mine, mine, ANY],
        out_shape=[array(blocks, ff, BLOCK), array(blocks, ff, BLOCK), array(*grad)],
        scratch_shapes=[vmem(d, ff, dtype=F32)] * 3 + [vmem(d, BLOCK), vmem(ff // PARTS // BLOCK, CORES, COLOURS, SIDE, *grad[-2:]), semaphores(SIDE)],
        args=(dy, silu, slope, b, act, wd), flops=8 * blocks * BLOCK * d * ff,
    )


def _loads(refs, layer):
    a, o, _, wo, wg, wu, wq, wk, wv = refs[10:19]
    *_, a_s, o_s, wo_s, wg_s, wu_s, wq_s, wk_s, wv_s, sems = refs
    pairs = [(r.at[layer], s) for r, s in ((wg, wg_s), (wu, wu_s), (wo, wo_s), (wq, wq_s), (wk, wk_s), (wv, wv_s), (a, a_s), (o, o_s))]
    return Loads(pairs[:3], sems, 0), Loads(pairs[3:], sems, 3)


def _open(*refs, layer):
    for loads in _loads(refs, layer):
        loads.start()


def _backward(*refs, flip, last, heads, steps, blocks, layer):
    first, rest = _loads(refs, layer)
    dg_ref, du_ref, h2_ref, dy_ref, q_ref, kv_ref, o_ref, lse_ref, tab_ref, tabs_ref, _, _, h = refs[:13]
    outs, refs = (refs[19:20], refs[20:]) if last else (refs[19:21], refs[21:])
    dh2_s, do_s, dq_s, dkv_s, k_s, v_s, acc_s, delta_s, dk_s, dv_s, gap_s, db_s, a_s, o_s, wo_s, wg_s, wu_s, wq_s, wk_s, wv_s, _ = refs
    step = pl.program_id(0)
    pairs = blocks * (blocks + 1) // 2
    @pl.when(step == 0)
    def _():
        gap(gap_s)
        k_s[...], v_s[...] = kv_ref[:HEAD, :].T, kv_ref[HEAD:, :].T
        dk_s[...], dv_s[...] = jnp.zeros_like(dk_s), jnp.zeros_like(dv_s)
        first.wait()

    @on(step, 0, steps)
    def _(n):
        here, part = at(lax.div(n, PARTS), BLOCK), at(lax.rem(n, PARTS), dg_ref.shape[0])
        db = dot(wg_s[:, part], get(dg_ref)) + dot(wu_s[:, part], get(du_ref))

        @pl.when(lax.rem(n, PARTS) == 0)
        def _():
            db_s[...] = db

        @pl.when(lax.rem(n, PARTS) > 0)
        def _():
            dh2 = norm_bwd(get(h2_ref), db + get(db_s), get(dy_ref).T if flip else get(dy_ref))
            dh2_s[:, here] = dh2
            do_s[:, here] = bf(dot(get(wo_s), dh2))

    @on(step, steps, pairs)
    def _(n):
        iq = query_block(n, blocks)
        j = n - lax.div(iq * (iq + 1), 2)
        scale = HEAD**-0.5
        e = scale * LOG2E
        mine = at(iq, BLOCK)
        rows = [slice(head * HEAD, head * HEAD + HEAD) for head in range(heads)]

        @pl.when(j == 0)
        def _():
            acc_s[...] = jnp.zeros_like(acc_s)
            for head, r in enumerate(rows):
                delta_s[head : head + 1, :] = (wide(do_s[r, mine]) * wide(o_ref[r, :])).sum(axis=0, keepdims=True)

        def block(start, size, skip, masked):
            here = pl.ds(pl.multiple_of(start, size), size)
            queries = pl.ds(pl.multiple_of(iq * BLOCK + skip, size), BLOCK - skip)
            keys, values, turned_keys = k_s[here, :], v_s[here, :], kv_ref[:HEAD, here]
            qs, dos, pairs_ = [q_ref[r, skip:] for r in rows], [do_s[r, queries] for r in rows], []
            for head in range(heads):
                for n in range(len(pairs_), min(head + AHEAD, heads)):
                    pairs_.append((dot(keys, qs[n]), dot(values, dos[n])))
                score, dp = pairs_[head]
                p = jnp.exp2(score * e - lse_ref[head : head + 1, skip:] * LOG2E)
                if masked:
                    p = jnp.where(gap_s[:, : BLOCK - skip] >= 0, p, 0.0)
                ds = bf(p * (dp - delta_s[head : head + 1, skip:]))
                dv_s[here, :] += dot_last(bf(p), dos[head])
                dk_s[here, :] += dot_last(ds, qs[head])
                acc_s[head, :, skip:] += dot(turned_keys, ds)

        pl.when(j < iq)(lambda: block(j * BLOCK, BLOCK, 0, False))

        @pl.when(j == iq)
        def _():
            for skip in range(0, BLOCK, FINE):
                block(iq * BLOCK + skip, FINE, skip, True)
            for head, r in enumerate(rows):
                dq_s[r, mine] = turned(bf(acc_s[head] * scale), get(tab_ref), True)

        @pl.when(n == pairs - 1)
        def _():
            dkv_s[:HEAD, :] = turned(bf((get(dk_s) * scale).T), get(tabs_ref), True)
            dkv_s[HEAD:, :] = bf(get(dv_s).T)
            rest.wait()

    if not last:
        @on(step, steps + pairs, blocks)
        def _(n):
            here = at(n, BLOCK)
            da = dot(get(wq_s), dq_s[:, here]) + dot(get(wk_s), dkv_s[:HEAD, here]) + dot(get(wv_s), dkv_s[HEAD:, here])
            outs[0][...] = norm_bwd(get(h), da, dh2_s[:, here])

    @pl.when(step == pl.num_programs(0) - 1)
    def _():
        grad_ref, n = outs[-1], 0
        for got in (dot_last(get(o_s), get(dh2_s)), dot_last(get(a_s), get(dq_s)), dot_last(get(a_s), get(dkv_s))):
            for c in range(0, got.shape[1], LANES):
                for r in range(0, got.shape[0], LANES):
                    grad_ref[n] = bf(got[r : r + LANES, c : c + LANES])
                    n += 1
        for n in range(n, PIECES):
            grad_ref[n] = jnp.zeros_like(grad_ref[n])


def query_block(n, blocks):
    return sum(jnp.where(n >= b * (b + 1) // 2, 1, 0) for b in range(1, blocks))


def backward(dg, du, dy, tab, kept, weights, layer, flip, last, comm, cid):
    a, q, kv, o, lse, h2, h = kept
    wq, wk, wv, wo, wg, wu = weights
    (_, d, t), ff = q.shape, dg.shape[1]
    heads, steps, blocks = d // HEAD, t // BLOCK * PARTS, t // BLOCK
    pairs = blocks * (blocks + 1) // 2
    more = 0 if last else blocks
    now, half = lambda i: lax.div(within(i, 0, steps), PARTS), lambda i: lax.rem(within(i, 0, steps), PARTS)
    block = lambda i: query_block(within(i, steps, pairs), blocks)
    then = lambda i: within(i, steps + pairs, blocks)
    hidden = pl.BlockSpec((None, ff // PARTS, BLOCK), lambda i: (now(i), half(i), 0))
    part = lambda rows, of: pl.BlockSpec((None, rows, BLOCK), lambda i: (layer, 0, of(i)))
    out_specs, out_shape = [pl.BlockSpec((PIECES, LANES, LANES), lambda i: (0, 0, 0))], [array(PIECES, LANES, LANES)]
    if not last:
        out_specs, out_shape = [cols(d, BLOCK, then)] + out_specs, [array(d, t)] + out_shape
    got = call(
        functools.partial(_backward, flip=flip, last=last, heads=heads, steps=steps, blocks=blocks, layer=layer), comm, cid, name="backward", opening=functools.partial(_open, layer=layer),
        grid=(steps + pairs + more + 1,),
        in_specs=[hidden, hidden, tiles(d, BLOCK, lambda i: (layer, now(i), 0)), pl.BlockSpec((BLOCK, d), lambda i: (now(i), 0)) if flip else cols(d, BLOCK, now),
                  part(d, block), pl.BlockSpec((None, *kv.shape[1:]), lambda i: (layer, 0, 0), pipeline_mode=pl.Buffered(1)), part(d, block), part(heads, block),
                  cols(HEAD, BLOCK, block), whole(HEAD, t), ANY, ANY, part(d, then)] + [ANY] * 6,
        out_specs=out_specs, out_shape=out_shape,
        scratch_shapes=[vmem(d, t), vmem(d, t), vmem(d, t), vmem(HEAD + HEAD, t), vmem(t, HEAD), vmem(t, HEAD), vmem(heads, HEAD, BLOCK, dtype=F32), vmem(heads, BLOCK, dtype=F32),
                        vmem(t, HEAD, dtype=F32), vmem(t, HEAD, dtype=F32), vmem(FINE, BLOCK, dtype=jnp.int32), vmem(d, BLOCK, dtype=F32), vmem(d, t), vmem(d, t)]
        + [vmem(*w.shape[1:]) for w in (wo, wg, wu, wq, wk, wv)] + [pltpu.SemaphoreType.DMA((8,))],
        args=(dg, du, h2, dy, q, kv, o, lse, tab, tab, a, o, h, wo, wg, wu, wq, wk, wv), flops=4 * t * d * (ff + t + d),
    )
    return (None if last else got[0]), got[0 if last else 1], got[1 if last else 2 :]


def stepped(w, m, v, g):
    m = 0.9 * m + 0.1 * g
    v = 0.95 * v + 0.05 * g * g
    return bf(w - 0.02 * (m * lax.rsqrt(v + 1e-8) + 0.1 * w)), m, v


def thirds(refs):
    return [refs[n : n + 7] for n in range(0, 21, 7)]


def rows_of(old, big, n):
    layer, way = len(big) - 1 - n // (2 * WAYS), n % WAYS
    z = 4 + n // WAYS % 2
    q = old[0][z].shape[1] // WAYS
    return z, (layer, pl.ds(way * q, q)), big[layer].at[way // COLOURS, way % COLOURS, :, :, pl.ds((z - 4) * q, q)]


def ahead(arrays, big, ready, sems):
    old, copies = thirds(arrays), []
    for n in range(READY):
        z, where, pieces = rows_of(old, big, n)
        for s, (src, to) in enumerate(zip([a[z].at[where] for a in old] + [pieces], ready)):
            copies.append(pltpu.make_async_copy(src, to.at[n], sems.at[n, s]))
    return copies


def _update(*refs, layers):
    old, refs = thirds(refs), refs[21:]
    big, small, ready, factor, refs = refs[:layers], refs[layers : 2 * layers], refs[2 * layers : 2 * layers + 4], refs[2 * layers + 4], refs[2 * layers + 5 :]
    new, refs = thirds(refs), refs[21:]
    buffers, (s_in, s_out) = [refs[n : n + 4] for n in range(0, 16, 4)], refs[16:]
    _, d, ff = old[0][4].shape
    q, tall, few = d // WAYS, d // LANES, LANES // WAYS
    f = factor[:1, :1]
    up = lambda g, i, c: g[c // SIDE, c % SIDE, at(i, TILE), :]
    panels = [(0, *rows_of(old, big, n), up) for n in range(2 * WAYS * layers)]
    for layer in range(layers):
        for way in range(WAYS):
            def down(g, i, c):
                n, part = lax.div(i, LANES // TILE), lax.rem(i, LANES // TILE)
                w, row = lax.div(part, few // TILE), lax.rem(part, few // TILE)
                return g[lax.div(w, COLOURS), lax.rem(w, COLOURS), n, pl.ds(pl.multiple_of(c * few + row * TILE, TILE), TILE), :]

            panels.append((1, 6, (layer, pl.ds(way * (ff // WAYS), ff // WAYS)), big[layer].at[:, :, way, :, pl.ds(2 * q, q)], down))
        first = 0
        for z in (3, 0, 1, 2):
            count = old[0][z].shape[2] // LANES * tall
            square = lambda g, i, c: g[c * tall + lax.div(i, LANES // TILE), at(lax.rem(i, LANES // TILE), TILE), :]
            panels.append((2 if count > tall else 3, z, (layer,), small[layer].at[pl.ds(first, count)], square))
            first += count
    alike = lambda n, end: sum(panels[m][0] == panels[n][0] for m in range(READY, end))
    order = sorted(range(READY, len(panels)), key=lambda n: (alike(n, n) + 0.5) / alike(n, len(panels)))
    used, jobs = [0] * len(buffers), []
    for kind, z, where, pieces, piece in panels[:READY] + [panels[n] for n in order]:
        slot = used[kind] % buffers[kind][0].shape[0]
        used[kind] += 1
        *held, g = [b.at[slot] for b in buffers[kind]]
        sems = lambda s, n: s.at[kind, slot, n]
        ins, source = [], held
        if len(jobs) < READY:
            *source, g = [r.at[len(jobs)] for r in ready]
        else:
            ins = [pltpu.make_async_copy(src, to, sems(s_in, n)) for n, (src, to) in enumerate(zip([a[z].at[where] for a in old] + [pieces], [*held, g]))]
        outs = [pltpu.make_async_copy(h, a[z].at[where], sems(s_out, n)) for n, (a, h) in enumerate(zip(new, held))]
        jobs.append(((kind, slot), ins, outs, source, held, g, piece))

    def work(source, held, g, piece):
        rows, columns = held[0].shape

        def body(i, _):
            here = at(i, TILE)
            for c in range(columns // LANES):
                part = slice(c * LANES, c * LANES + LANES)
                got = stepped(*(wide(h[here, part]) for h in source), wide(piece(g, i, c)) * f)
                for h, value in zip(held, got):
                    h[here, part] = value
            return _

        lax.fori_loop(0, rows // TILE, body, 0)

    busy, waiting, started = set(), [], set()

    def load(n):
        if n not in started and jobs[n][0] not in busy:
            for copy in jobs[n][1]:
                copy.start()
            busy.add(jobs[n][0])
            started.add(n)

    for n, (slot, ins, outs, source, held, g, piece) in enumerate(jobs):
        for m in range(n, len(jobs)):
            load(m)
        for copy in ins:
            copy.wait()
        work(source, held, g, piece)
        for copy in outs:
            copy.start()
        waiting.append(n)
        for m in waiting[:-2] if n + 1 < len(jobs) else waiting:
            for copy in jobs[m][2]:
                copy.wait()
            busy.discard(jobs[m][0])
        waiting = waiting[-2:]


def update(arrays, big, small, ready, factor):
    layers, d, ff = arrays[4].shape
    kv, q, tall = arrays[1].shape[2], d // WAYS, d // LANES
    small = [s.reshape(-1, LANES, LANES) for s in small]
    given = kept_in(pltpu.HBM, *arrays, *big, *small) + kept_in(pltpu.VMEM, *ready, factor)
    kinds = [(3, (q, ff), (SIDE, SIDE, q, LANES)), (3, (ff // WAYS, d), (CORES, COLOURS, SIDE, q, LANES)), (1, (d, d), (tall * tall, LANES, LANES)), (1, (d, kv), (tall, LANES, LANES))]
    scratch = [vmem(n, *s, dtype=t) for n, panel, pieces in kinds for s, t in ((panel, BF), (panel, F32), (panel, F32), (pieces, BF))]
    return pl.pallas_call(
        functools.partial(_update, layers=layers), name="update", in_specs=[HBM] * (21 + 2 * layers) + [HERE] * 5, out_specs=[ANY] * 21,
        out_shape=[array(*a.shape, dtype=a.dtype) for a in arrays], scratch_shapes=scratch + [semaphores(4, 4, 4), semaphores(4, 4, 3)],
        compiler_params=pltpu.CompilerParams(vmem_limit_bytes=33 * 2**20), cost_estimate=cost(2**28),
    )(*given)


def _finish(pieces, *refs, count, shards):
    shards, arrays, big, refs = refs[:shards], refs[shards : shards + 21], refs[shards + 21 : shards + 23], refs[shards + 23 :]
    back, factor, *ready = refs[:6]
    shard, s_ready, *scratch = refs[6:]
    place = Place()
    copies = ahead(arrays, big, ready, s_ready)
    *sums, s_sums = scratch[:4]
    scratch, sums = scratch[4:], Loads(list(zip(shards, sums)), s_sums, 0)
    sums.start()
    reduce, gather = Reduce(place, pieces, shard, scratch[:8]), Gather(place, shard, back, scratch[8:12])
    pair, line, s_pair, s_line = scratch[12:]
    place.greet()
    reduce.start()
    sums.wait()
    total = sum(squares(copy.dst_ref) for copy in sums.copies)
    for copy in copies:
        copy.start()
    for stage in reduce.stages()[1:]:
        stage()
    gather.start()
    total = total + squares(shard)
    pair[place.core] = total
    loads = copies
    rounds = [[send(pair.at[place.core], pair.at[place.core], s_pair, (0,), place.partner())]]
    for axis in range(COLOURS):
        mine = line.at[axis, place.places[axis]]
        rounds.append([send(mine, mine, s_line, (axis, far), place.along(axis, far)) for far in FAR])
    for n, (copies, stage) in enumerate(zip(rounds, (gather.first, gather.relay, gather.second))):
        if n:
            line[n - 1, place.places[n - 1]] = total
        for copy in copies:
            copy.start()
        for copy in copies:
            copy.wait()
        total = sum(line[n - 1, m] for m in range(SIDE)) if n else sum(pair[m] for m in range(CORES))
        stage()
    factor[...] = jnp.broadcast_to(jnp.minimum(ONE, 0.5 * lax.rsqrt(jnp.sum(total, keepdims=True) / count + 1e-30)), factor.shape)
    gather.finish()
    for copy in loads:
        copy.wait()


def finish(pieces, shards, arrays, big, cid, count):
    rows, (_, d, ff) = pieces.shape[-2], arrays[4].shape
    q = d // WAYS
    ready = [pltpu.VMEM((READY, *s), t) for s, t in (((q, ff), BF), ((q, ff), F32), ((q, ff), F32), ((SIDE, SIDE, q, LANES), BF))]
    return pl.pallas_call(
        functools.partial(_finish, count=count, shards=len(shards)), name="finish", in_specs=[HBM] * (1 + len(shards) + len(arrays) + len(big)),
        out_specs=[HBM] + [HERE] * 5, out_shape=[pltpu.HBM(pieces.shape, BF), pltpu.VMEM((TILE, LANES), F32)] + ready,
        scratch_shapes=[vmem(COLOURS, rows, LANES), semaphores(READY, 4)] + [vmem(*s.shape) for s in shards] + [semaphores(len(shards))] + Reduce.scratch(rows) + Gather.scratch(rows)
        + [vmem(CORES, TILE, LANES, dtype=F32), vmem(COLOURS, SIDE, TILE, LANES, dtype=F32), semaphores(2, 1), semaphores(2, COLOURS, SIDE)],
        compiler_params=pltpu.CompilerParams(collective_id=cid, has_side_effects=True, vmem_limit_bytes=20 * 2**20), cost_estimate=cost(2**24),
    )(*kept_in(pltpu.HBM, pieces, *shards, *arrays, *big))


def solution(mesh):
    def step(x, dy, *arrays):
        wq, wk, wv, wo, wg, wu, wd = weights = arrays[:7]
        tab = jnp.asarray(rotary(x.shape[1]))
        h, a, q, kv, o, lse, h2, b, silu, slope, act = forward(x[0], tab, *weights)
        kept, mine = (a, q, kv, o, lse, h2, h), (wq, wk, wv, wo, wg, wu)
        cut = lambda g: g.reshape(CORES, COLOURS, SIDE, SIDE, LANES, LANES)
        dg, du, big = gradients(dy[0], silu, slope, b, act, wd, 1, True, None, 0)
        comm = Comm(big, (0, 1, 6, 9, 11, 11, 13, 17, 20, -23))
        dh, small, (s1, big1) = backward(dg, du, dy[0], tab, kept, mine, 1, True, False, comm, 1)
        comm = Comm(cut(small), (0, 1, 2, 3, 4, 4, 5, 6, 7, -8))
        dg, du, big, s2, small1 = gradients(dh, silu, slope, b, act, wd, 0, False, comm, 2)
        comm = Comm(big, (0, 1, 6, 9, 11, 11, 13, 17, -19, -19))
        _, small, (s3, big0) = backward(dg, du, dh, tab, kept, mine, 0, False, True, comm, 3)
        small0, factor, *ready = finish(cut(small), (s1, s2, s3), arrays, (big0, big1), 4, sum(w.size for w in weights))
        return tuple(update(arrays, [big0, big1], [small0, small1], ready, factor))

    states, all_of = P(("rep", "dp"), None, None), P(None, None, None)
    return jax.shard_map(step, mesh=mesh, in_specs=(states,) * 2 + (all_of,) * 21, out_specs=(P("rep", None, None),) * 21, check_vma=False)
```
